32 devices in a mesh: tm: 4 (over y, x), rows: 2 (over core), batch: 4 (over z).
Axes of the slice: x: 2, y: 2, z: 4, core: 2. Of those that a mesh axis runs over, the one named last changes fastest.
Arguments:
- inputs: bfloat16 [4, 8, 16, 128, 384], P('batch', 'tm', 'rows'), parts along dimension 0, may hold values from -16 to 16
- norm_gain: float32 [384], replicated, may hold values from 0.1 to 1.9
- norm_bias: float32 [384], replicated, may hold values from -3 to 3
- conv_weight: bfloat16 [3, 3, 3, 384, 384], replicated, may hold values from -0.0625 to 0.0625
- conv_bias: float32 [384], replicated, may hold values from -2 to 2
Outputs:
- decoded: bfloat16 [4, 8, 16, 128, 384], P('batch', 'tm', 'rows'), parts along dimension 0
The draws below stay inside these ranges and needn't reach their ends.
There are 4 independent parts, one for each index of `batch`. The reference program is written for one: setup_inputs(seed, part) draws one part's arguments, and reference() takes and returns one part's arrays. A program takes and returns all parts, laid end to end along the dimension named above; an argument that names none is the same for every part. Nothing has to cross between parts.
All inputs are finite; a program needn't handle non-finite values.
Results may differ from the reference program's by a relative error of at most 0.0025.
Values may be sent and summed in bfloat16 or wider, within the bound.
A program may use at most 128 MiB of HBM per device.

```python
import jax
import jax.numpy as jnp
from jax import lax

CHANNELS = 384
GROUPS = 32
WIDTH = 128
CLIPS = 1
FRAMES = 8
HEIGHT = 16


def draw_inputs(key, part):
    subkeys = jax.random.split(jax.random.fold_in(key, 17), 4)
    full_shape = (CLIPS, FRAMES, HEIGHT, WIDTH, CHANNELS)
    scales = 0.6 * jnp.exp(jax.random.uniform(subkeys[0], (CLIPS, FRAMES, HEIGHT, 1, 1), jnp.float32, -1.2, 1.2))
    offsets = 1.2 + 0.4 * jax.random.truncated_normal(subkeys[1], -5.0, 5.0, (CHANNELS,), jnp.float32)
    row_place = (jnp.arange(HEIGHT, dtype=jnp.float32) + 0.5) / HEIGHT
    row_ramp = (3.0 * row_place - 1.5).reshape(1, 1, HEIGHT, 1, 1)
    frame_level = jax.random.uniform(subkeys[3], (CLIPS, FRAMES, 1, 1, 1), jnp.float32, -1.2, 1.2)
    region = row_ramp + frame_level
    noisy_part = jax.random.truncated_normal(subkeys[2], -4.0, 4.0, full_shape, jnp.float32)
    values = noisy_part * scales + offsets + region
    return values.astype(jnp.bfloat16)


def bell_draw(key, extent, scale, limit, kind=jnp.bfloat16):
    values = jax.random.normal(key, extent, jnp.float32) * scale
    return jnp.minimum(jnp.maximum(values, -limit), limit).astype(kind)


def setup_inputs(seed: int = 0, part: int = 0) -> dict:
    key_list = jax.random.split(jax.random.key(seed), 6)
    own_keys = jax.random.split(jax.random.fold_in(key_list[5], part), 6)
    return {
        "inputs": draw_inputs(jax.random.fold_in(jax.random.fold_in(key_list[5], part), 71), part),
        "norm_gain": jnp.clip(1.0 + 0.18 * jax.random.normal(key_list[1], (CHANNELS,), jnp.float32), 0.1, 1.9),
        "norm_bias": bell_draw(key_list[2], (CHANNELS,), 0.5, 3.0, jnp.float32),
        "conv_weight": bell_draw(key_list[3], (3, 3, 3, CHANNELS, CHANNELS), (27 * CHANNELS) ** -0.5, 0.0625),
        "conv_bias": bell_draw(key_list[4], (CHANNELS,), 0.3, 2.0, jnp.float32),
    }


epsilon = 1e-06

def convolve(padded, conv_weight, frames, height, width):
    channels = padded.shape[-1]
    summed = jnp.zeros((padded.shape[0] * frames * height * width, conv_weight.shape[-1]), jnp.float32)
    for tap_time in range(3):
        for tap_row in range(3):
            slab_rows = padded[:, tap_time:tap_time + frames, tap_row:tap_row + height]
            columns = jnp.concatenate([slab_rows[:, :, :, 0:width], slab_rows[:, :, :, 1:width + 1], slab_rows[:, :, :, 2:width + 2]], axis=-1)
            kernel = conv_weight[tap_time, tap_row].reshape(3 * channels, -1)
            summed = summed + jnp.dot(columns.reshape(-1, 3 * channels), kernel, preferred_element_type=jnp.float32)
    return summed

def reference(inputs, norm_gain, norm_bias, conv_weight, conv_bias):
    values = inputs.astype(jnp.float32)
    channels = values.shape[-1]
    per_group = channels // GROUPS
    cell_count = 1.0 * CLIPS * FRAMES * HEIGHT * WIDTH * per_group
    chan_sum = lax.optimization_barrier(jnp.sum(values, axis=(0, 1, 2, 3)))
    group_mean = lax.optimization_barrier(jnp.sum(chan_sum.reshape(GROUPS, per_group), axis=1)) / cell_count
    centered = values - jnp.repeat(group_mean, per_group)
    chan_square = lax.optimization_barrier(jnp.sum(centered * centered, axis=(0, 1, 2, 3)))
    group_var = lax.optimization_barrier(jnp.sum(chan_square.reshape(GROUPS, per_group), axis=1)) / cell_count
    inverse = jnp.repeat(lax.rsqrt(group_var + epsilon), per_group)
    normed = centered * inverse * norm_gain + norm_bias
    active = (normed * jax.nn.sigmoid(normed)).astype(jnp.bfloat16)
    padded = jnp.pad(active, ((0, 0), (2, 0), (1, 1), (1, 1), (0, 0)))
    summed = convolve(padded, conv_weight, FRAMES, HEIGHT, WIDTH)
    result = values + summed.reshape(values.shape) + conv_bias
    return result.astype(jnp.bfloat16)
```

```python
import functools

import jax
import jax.numpy as jnp
from jax import lax
from jax.experimental import pallas as pl
from jax.experimental.pallas import tpu as pltpu
from jax.sharding import PartitionSpec as P

GROUPS = 32
MESH = pl.DeviceIdType.MESH
OWN_ROWS = 4

epsilon = 1e-06


def block_kernel(
    T, R, x_hbm, gain_hbm, nbias_hbm, w_hbm, cbias_hbm, out_ref,
    params, p_sem, xv, wv, hraw, eown, ehalo, own3, halo3, edge3, acc, stats,
    x_sem, w_sem, halo_send, halo_recv, eown_send, eown_recv,
    ehalo_send, ehalo_recv, stat_send, stat_recv,
):
    F, H, W, C = x_hbm.shape
    C3 = 3 * C
    n = T * R
    tm = lax.axis_index("tm")
    row = lax.axis_index("rows")
    me = tm * R + row

    def peer(offset):
        other = lax.rem(me + offset, n)
        return {"tm": other // R, "rows": lax.rem(other, R)}

    x_copies = [pltpu.make_async_copy(x_hbm.at[f], xv.at[f], x_sem.at[f]) for f in range(F)]
    w_copies = [
        pltpu.make_async_copy(
            w_hbm.at[kt, kh], wv.at[kt, :, pl.ds(kh * C, C)], w_sem.at[kt * 3 + kh]
        )
        for kt in range(3)
        for kh in range(3)
    ]
    p_copies = [
        pltpu.make_async_copy(p, params.at[k, 0], p_sem.at[k])
        for k, p in enumerate((gain_hbm, nbias_hbm, cbias_hbm))
    ]
    barrier = pltpu.get_barrier_semaphore()
    for d in range(1, n):
        pl.semaphore_signal(barrier, inc=1, device_id=peer(d), device_id_type=MESH)
    for c in x_copies + p_copies:
        c.start()
    def row_of(i):
        return jnp.where(i == 0, 0, jnp.where(i == 1, H - 1, i - 1))

    def halo_copy(i, r):
        return pltpu.make_async_remote_copy(
            src_ref=xv.at[pl.ds(F - 2, 2), pl.ds(r, 1)],
            dst_ref=hraw.at[:, pl.ds(r, 1)],
            send_sem=halo_send.at[i],
            recv_sem=halo_recv.at[i],
            device_id={"tm": lax.rem(tm + 1, T), "rows": row},
            device_id_type=MESH,
        )

    def last_copy(f):
        return pltpu.make_async_remote_copy(
            src_ref=xv.at[F - 2 + f, H - 2],
            dst_ref=hraw.at[f, H - 2],
            send_sem=halo_send.at[H - 1 + f],
            recv_sem=halo_recv.at[H - 1 + f],
            device_id={"tm": lax.rem(tm + 1, T), "rows": row},
            device_id_type=MESH,
        )

    def own_edge(side):
        r = H - 1 if side == 0 else 0
        target = row + 1 if side == 0 else row - 1
        return pltpu.make_async_remote_copy(
            src_ref=xv.at[:, pl.ds(r, 1)],
            dst_ref=eown.at[side],
            send_sem=eown_send.at[side],
            recv_sem=eown_recv.at[side],
            device_id={"tm": tm, "rows": lax.rem(target + R, R)},
            device_id_type=MESH,
        )

    def halo_edge(side):
        r = H - 1 if side == 0 else 0
        target = row + 1 if side == 0 else row - 1
        return pltpu.make_async_remote_copy(
            src_ref=hraw.at[:, pl.ds(r, 1)],
            dst_ref=ehalo.at[side],
            send_sem=ehalo_send.at[side],
            recv_sem=ehalo_recv.at[side],
            device_id={"tm": tm, "rows": lax.rem(target + R, R)},
            device_id_type=MESH,
        )

    has_next, has_prev = tm < T - 1, tm > 0
    sends_edge = (row < R - 1, row > 0)
    gets_edge = (row > 0, row < R - 1)

    for c in w_copies:
        c.start()

    total = jnp.zeros((8, C), jnp.float32)
    square = jnp.zeros((8, C), jnp.float32)
    for f in range(F):
        x_copies[f].wait()

        def add_rows(r, carry):
            v = xv[f, r].astype(jnp.float32).reshape(W // 8, 8, C)
            return carry[0] + jnp.sum(v, axis=0), carry[1] + jnp.sum(v * v, axis=0)

        total, square = lax.fori_loop(0, H, add_rows, (total, square))
    stats[0, 0:1] = jnp.sum(total, axis=0, keepdims=True)
    stats[0, 1:2] = jnp.sum(square, axis=0, keepdims=True)
    pl.semaphore_wait(barrier, n - 1)

    def stat_copy(d):
        return pltpu.make_async_remote_copy(
            src_ref=stats.at[0],
            dst_ref=stats.at[d],
            send_sem=stat_send.at[d],
            recv_sem=stat_recv.at[d],
            device_id=peer(d),
            device_id_type=MESH,
        )

    for d in range(1, n):
        stat_copy(d).start()

    @pl.when(has_next)
    def _():
        for i in range(H - 1):
            halo_copy(i, 0 if i == 0 else H - 1 if i == 1 else i - 1).start()
        for f in (1, 0):
            last_copy(f).start()

    for side in range(2):
        @pl.when(sends_edge[side])
        def _():
            own_edge(side).start()

    for c in p_copies:
        c.wait()
    for f in range(F):
        def start_acc(r, _):
            acc[f, r + 1] = xv[f, r].astype(jnp.float32) + params[2]
            return 0

        lax.fori_loop(0, H, start_acc, 0)
    for d in range(1, n):
        stat_copy(d).wait_recv()
    total = stats[0]
    for d in range(1, n):
        total = total + stats[d]
    sums = jnp.concatenate(
        [
            jnp.broadcast_to(total[0:1], (8, C)),
            jnp.broadcast_to(total[1:2], (8, C)),
        ],
        axis=0,
    )
    per_group = C // GROUPS
    channel = lax.broadcasted_iota(jnp.int32, (C, C), 0)
    other = lax.broadcasted_iota(jnp.int32, (C, C), 1)
    first = (other // per_group) * per_group
    member = jnp.where((channel >= first) & (channel < first + per_group), 1.0, 0.0)
    cells = 1.0 * F * H * W * per_group * n
    moments = (
        jnp.dot(
            sums,
            member.astype(jnp.float32),
            preferred_element_type=jnp.float32,
            precision=lax.Precision.HIGHEST,
        )
        / cells
    )
    mean = moments[0:1]
    var = jnp.maximum(moments[8:9] - mean * mean, 0.0)
    half_scale = lax.rsqrt(var + epsilon) * params[0] * 0.5
    half_bias = params[1] * 0.5

    column = lax.broadcasted_iota(jnp.int32, (W, C), 0)

    def activate(raw, put):
        h = (raw.astype(jnp.float32) - mean) * half_scale + half_bias
        a = h + h * jnp.tanh(h)
        put(0, jnp.where(column == 0, 0.0, pltpu.roll(a, 1, 0)).astype(jnp.bfloat16))
        put(1, a.astype(jnp.bfloat16))
        put(2, jnp.where(column == W - 1, 0.0, pltpu.roll(a, W - 1, 0)).astype(jnp.bfloat16))

    for f in range(F):
        def own_row(r, _):
            def put(k, v):
                own3[f, r, :, k * C : (k + 1) * C] = v

            activate(xv[f, r], put)
            return 0

        lax.fori_loop(0, H, own_row, 0)

    @pl.when(has_prev)
    def _():
        for i in range(2):
            halo_copy(i, 0 if i == 0 else H - 1).wait_recv()
        for side in range(2):
            @pl.when(sends_edge[side])
            def _():
                halo_edge(side).start()

    for c in w_copies:
        c.wait()

    def product(lhs, kt, lo=0, hi=3):
        return jnp.dot(
            lhs, wv[kt, :, lo * C : hi * C], preferred_element_type=jnp.float32
        )

    def finish(r, _):
        for f in range(F):
            out_ref[f, r] = acc[f, r + 1].astype(out_ref.dtype)
        return 0

    def own_rows(g, _):
        r0 = g * OWN_ROWS
        for kt in range(3):
            count = F - 2 + kt
            if count <= 0:
                continue
            lhs = own3[0:count, pl.ds(r0, OWN_ROWS)].reshape(count * OWN_ROWS * W, C3)
            y = product(lhs, kt)
            for kh in range(3):
                part = y[:, kh * C : (kh + 1) * C].reshape(count, OWN_ROWS, W, C)
                acc[2 - kt : 2 - kt + count, pl.ds(r0 + 2 - kh, OWN_ROWS)] += part
        return 0

    lax.fori_loop(0, H // OWN_ROWS, own_rows, 0)

    for side in range(2):
        kh = 0 if side == 0 else 2
        at = 1 if side == 0 else H

        @pl.when(gets_edge[side])
        def _():
            own_edge(side).wait_recv()
            for f in range(F):
                def put(k, v):
                    edge3[f, :, k * C : (k + 1) * C] = v

                activate(eown[side, f, 0], put)
            for kt in range(3):
                count = F - 2 + kt
                if count > 0:
                    lhs = edge3[0:count].reshape(count * W, C3)
                    acc[2 - kt : 2 - kt + count, at] += product(lhs, kt, kh, kh + 1).reshape(
                        count, W, C
                    )

    @pl.when(has_prev)
    def _():
        def halo_row(i, _):
            r = row_of(i)

            @pl.when(i >= 2)
            def _():
                halo_copy(i, r).wait_recv()

            for f in range(2):
                def put(k, v):
                    halo3[f, :, k * C : (k + 1) * C] = v

                activate(hraw[f, r], put)
            y = product(halo3[...].reshape(2 * W, C3), 0)
            z = product(halo3[1], 1)
            for kh in range(3):
                cols = slice(kh * C, (kh + 1) * C)
                acc[0, r + 2 - kh] += y[:W, cols] + z[:, cols]
                acc[1, r + 2 - kh] += y[W:, cols]

            @pl.when(i >= 2)
            def _():
                finish(i - 2, 0)

            return 0

        lax.fori_loop(0, 2, halo_row, 0)
        for side in range(2):
            kh = 0 if side == 0 else 2
            at = 1 if side == 0 else H

            @pl.when(gets_edge[side])
            def _():
                halo_edge(side).wait_recv()
                for f in range(2):
                    def put(k, v):
                        halo3[f, :, k * C : (k + 1) * C] = v

                    activate(ehalo[side, f, 0], put)
                y = product(halo3[...].reshape(2 * W, C3), 0, kh, kh + 1)
                z = product(halo3[1], 1, kh, kh + 1)
                acc[0, at] += y[:W] + z
                acc[1, at] += y[W:]

        lax.fori_loop(2, H - 1, halo_row, 0)

        r = H - 2
        for f in (1, 0):
            last_copy(f).wait_recv()

            def put(k, v):
                halo3[f, :, k * C : (k + 1) * C] = v

            activate(hraw[f, r], put)
            y = product(halo3[f], 0)
            if f == 1:
                z = product(halo3[f], 1)
                for kh in range(3):
                    acc[0, r + 2 - kh] += z[:, kh * C : (kh + 1) * C]
            for kh in range(3):
                out_ref[f, r + 1 - kh] = (
                    acc[f, r + 2 - kh] + y[:, kh * C : (kh + 1) * C]
                ).astype(out_ref.dtype)

    @pl.when(jnp.logical_not(has_prev))
    def _():
        lax.fori_loop(0, H, finish, 0)

    for d in range(1, n):
        stat_copy(d).wait_send()

    @pl.when(has_next)
    def _():
        for i in range(H - 1):
            halo_copy(i, 0 if i == 0 else H - 1 if i == 1 else i - 1).wait_send()
        for f in (1, 0):
            last_copy(f).wait_send()

    for side in range(2):
        @pl.when(sends_edge[side])
        def _():
            own_edge(side).wait_send()

            @pl.when(has_prev)
            def _():
                halo_edge(side).wait_send()


def shards(T, R, inputs, norm_gain, norm_bias, conv_weight, conv_bias):
    _, F, H, W, C = inputs.shape
    n = T * R

    def pin(a):
        return pltpu.with_memory_space_constraint(a, pltpu.HBM)

    vmem = pl.BlockSpec(memory_space=pltpu.VMEM)
    hbm = pl.BlockSpec(memory_space=pltpu.HBM)
    anywhere = pl.BlockSpec(memory_space=pl.ANY)
    dma = pltpu.SemaphoreType.DMA
    out = pl.pallas_call(
        functools.partial(block_kernel, T, R),
        out_shape=jax.ShapeDtypeStruct((F, H, W, C), inputs.dtype),
        in_specs=[hbm, anywhere, anywhere, hbm, anywhere],
        out_specs=vmem,
        scratch_shapes=[
            pltpu.VMEM((3, 1, C), jnp.float32),
            dma((3,)),
            pltpu.VMEM((F, H, W, C), jnp.bfloat16),
            pltpu.VMEM((3, 3 * C, 3 * C), jnp.bfloat16),
            pltpu.VMEM((2, H, W, C), jnp.bfloat16),
            pltpu.VMEM((2, F, 1, W, C), jnp.bfloat16),
            pltpu.VMEM((2, 2, 1, W, C), jnp.bfloat16),
            pltpu.VMEM((F, H, W, 3 * C), jnp.bfloat16),
            pltpu.VMEM((2, W, 3 * C), jnp.bfloat16),
            pltpu.VMEM((F, W, 3 * C), jnp.bfloat16),
            pltpu.VMEM((F, H + 2, W, C), jnp.float32),
            pltpu.VMEM((n, 2, C), jnp.float32),
            dma((F,)),
            dma((9,)),
            dma((H + 1,)),
            dma((H + 1,)),
            dma((2,)),
            dma((2,)),
            dma((2,)),
            dma((2,)),
            dma((n,)),
            dma((n,)),
        ],
        compiler_params=pltpu.CompilerParams(
            collective_id=0, has_side_effects=True, vmem_limit_bytes=50 * 1024 * 1024
        ),
        name="norm_conv_block",
    )(
        pin(inputs.reshape(F, H, W, C)),
        pin(norm_gain),
        pin(norm_bias),
        pin(conv_weight.reshape(3, 3, 3 * C, C)),
        pin(conv_bias),
    )
    return out.reshape(inputs.shape)


def solution(mesh):
    placed = (P("batch", "tm", "rows", None, None), P(), P(), P(), P())
    return jax.shard_map(
        functools.partial(shards, mesh.shape["tm"], mesh.shape["rows"]),
        mesh=mesh,
        in_specs=placed,
        out_specs=P("batch", "tm", "rows", None, None),
        check_vma=False,
    )
```

```python
import functools

import jax
import jax.numpy as jnp
from jax import lax
from jax.experimental import pallas as pl
from jax.experimental.pallas import tpu as pltpu
from jax.sharding import PartitionSpec as P

GROUPS = 32
MESH = pl.DeviceIdType.MESH
OWN_ROWS = 4

epsilon = 1e-06


def block_kernel(
    T, R, x_hbm, gain_hbm, nbias_hbm, w_hbm, cbias_hbm, out_ref,
    params, p_sem, xv, wv, hraw, eown, ehalo, own3, halo3, edge3, acc, stats,
    x_sem, w_sem, halo_send, halo_recv, eown_send, eown_recv,
    ehalo_send, ehalo_recv, stat_send, stat_recv, fwd_send, relayed, relay_sem,
):
    F, H, W, C = x_hbm.shape
    C3 = 3 * C
    n = T * R
    tm = lax.axis_index("tm")
    row = lax.axis_index("rows")
    me = tm * R + row

    def peer(offset):
        other = lax.rem(me + offset, n)
        return {"tm": other // R, "rows": lax.rem(other, R)}

    def far(a, b):
        return (a == T - 1) & (b == 0) & (T > 2)

    def tm_of(d):
        return lax.rem(me + n - d, n) // R

    x_copies = [pltpu.make_async_copy(x_hbm.at[f], xv.at[f], x_sem.at[f]) for f in range(F)]
    w_copies = [
        pltpu.make_async_copy(
            w_hbm.at[kt, kh], wv.at[kt, :, pl.ds(kh * C, C)], w_sem.at[kt * 3 + kh]
        )
        for kt in range(3)
        for kh in range(3)
    ]
    p_copies = [
        pltpu.make_async_copy(p, params.at[k, 0], p_sem.at[k])
        for k, p in enumerate((gain_hbm, nbias_hbm, cbias_hbm))
    ]
    barrier = pltpu.get_barrier_semaphore()
    for d in range(1, n):
        other = peer(d)

        @pl.when(jnp.logical_not(far(tm, other["tm"])))
        def _():
            pl.semaphore_signal(barrier, inc=1, device_id=other, device_id_type=MESH)
    for c in x_copies + p_copies:
        c.start()
    def row_of(i):
        return jnp.where(i == 0, 0, jnp.where(i == 1, H - 1, i - 1))

    def halo_copy(i, r):
        return pltpu.make_async_remote_copy(
            src_ref=xv.at[pl.ds(F - 2, 2), pl.ds(r, 1)],
            dst_ref=hraw.at[:, pl.ds(r, 1)],
            send_sem=halo_send.at[i],
            recv_sem=halo_recv.at[i],
            device_id={"tm": lax.rem(tm + 1, T), "rows": row},
            device_id_type=MESH,
        )

    relay_in = pltpu.make_async_remote_copy(
        src_ref=xv.at[pl.ds(F - 2, 2), pl.ds(H - 3, 1)],
        dst_ref=relayed,
        send_sem=relay_sem.at[0],
        recv_sem=relay_sem.at[1],
        device_id={"tm": T - 1, "rows": row},
        device_id_type=MESH,
    )
    relay_out = pltpu.make_async_remote_copy(
        src_ref=relayed,
        dst_ref=hraw.at[:, pl.ds(H - 3, 1)],
        send_sem=relay_sem.at[2],
        recv_sem=halo_recv.at[H - 2],
        device_id={"tm": max(T - 2, 0), "rows": row},
        device_id_type=MESH,
    )

    def last_copy(f):
        return pltpu.make_async_remote_copy(
            src_ref=xv.at[F - 2 + f, H - 2],
            dst_ref=hraw.at[f, H - 2],
            send_sem=halo_send.at[H - 1 + f],
            recv_sem=halo_recv.at[H - 1 + f],
            device_id={"tm": lax.rem(tm + 1, T), "rows": row},
            device_id_type=MESH,
        )

    def own_edge(side):
        r = H - 1 if side == 0 else 0
        target = row + 1 if side == 0 else row - 1
        return pltpu.make_async_remote_copy(
            src_ref=xv.at[:, pl.ds(r, 1)],
            dst_ref=eown.at[side],
            send_sem=eown_send.at[side],
            recv_sem=eown_recv.at[side],
            device_id={"tm": tm, "rows": lax.rem(target + R, R)},
            device_id_type=MESH,
        )

    def halo_edge(side):
        r = H - 1 if side == 0 else 0
        target = row + 1 if side == 0 else row - 1
        return pltpu.make_async_remote_copy(
            src_ref=hraw.at[:, pl.ds(r, 1)],
            dst_ref=ehalo.at[side],
            send_sem=ehalo_send.at[side],
            recv_sem=ehalo_recv.at[side],
            device_id={"tm": tm, "rows": lax.rem(target + R, R)},
            device_id_type=MESH,
        )

    has_next, has_prev = tm < T - 1, tm > 0
    relays, relayed_by = (tm == T - 1) & (T == 4), (tm == T - 3) & (T == 4)
    sends_edge = (row < R - 1, row > 0)
    gets_edge = (row > 0, row < R - 1)

    total = jnp.zeros((8, C), jnp.float32)
    square = jnp.zeros((8, C), jnp.float32)
    for f in range(F):
        if f == 0:
            x_copies[f].wait()

        def add_rows(r, carry):
            v = xv[f, r].astype(jnp.float32).reshape(W // 8, 8, C)
            return carry[0] + jnp.sum(v, axis=0), carry[1] + jnp.sum(v * v, axis=0)

        total, square = lax.fori_loop(0, H, add_rows, (total, square))
        if f == 0:
            for g in range(1, F):
                x_copies[g].wait()
            first = far(T - 1, tm)

            @pl.when(first)
            def _():
                pl.semaphore_wait(barrier, n - 1 - R)

            @pl.when(jnp.logical_not(first))
            def _():
                pl.semaphore_wait(barrier, n - 1)

            @pl.when(has_next)
            def _():
                halo_copy(0, 0).start()

            for c in w_copies:
                c.start()


    stats[0, 0:1] = jnp.sum(total, axis=0, keepdims=True)
    stats[0, 1:2] = jnp.sum(square, axis=0, keepdims=True)

    def stat_copy(d):
        return pltpu.make_async_remote_copy(
            src_ref=stats.at[0],
            dst_ref=stats.at[d],
            send_sem=stat_send.at[d],
            recv_sem=stat_recv.at[d],
            device_id=peer(d),
            device_id_type=MESH,
        )

    for d in range(1, n):
        @pl.when(jnp.logical_not(far(peer(d)["tm"], tm)))
        def _():
            stat_copy(d).start()

    @pl.when(has_next)
    def _():
        for i in range(1, H - 2):
            halo_copy(i, H - 1 if i == 1 else i - 1).start()

        @pl.when(relayed_by)
        def _():
            relay_in.start()

        @pl.when(jnp.logical_not(relayed_by))
        def _():
            halo_copy(H - 2, H - 3).start()

        for f in (1, 0):
            last_copy(f).start()

    for side in range(2):
        @pl.when(sends_edge[side])
        def _():
            own_edge(side).start()

    def stat_forward(r):
        d = (T - 1) * R + r - row
        return pltpu.make_async_remote_copy(
            src_ref=stats.at[R],
            dst_ref=stats.at[d],
            send_sem=fwd_send.at[r],
            recv_sem=stat_recv.at[d],
            device_id={"tm": T - 1, "rows": r},
            device_id_type=MESH,
        )

    second = (tm == 1) & (T > 2)

    @pl.when(second)
    def _():
        stat_copy(R).wait_recv()
        for r in range(R):
            stat_forward(r).start()

    for c in p_copies:
        c.wait()
    for f in range(F):
        def start_acc(r, _):
            acc[f, r + 1] = xv[f, r].astype(jnp.float32) + params[2]
            return 0

        lax.fori_loop(0, H, start_acc, 0)
    for d in range(1, n):
        if d == R:
            @pl.when(jnp.logical_not(second))
            def _():
                stat_copy(d).wait_recv()
        else:
            stat_copy(d).wait_recv()
    total = stats[0]
    for d in range(1, n):
        total = total + stats[d]
    sums = jnp.concatenate(
        [
            jnp.broadcast_to(total[0:1], (8, C)),
            jnp.broadcast_to(total[1:2], (8, C)),
        ],
        axis=0,
    )
    per_group = C // GROUPS
    channel = lax.broadcasted_iota(jnp.int32, (C, C), 0)
    other = lax.broadcasted_iota(jnp.int32, (C, C), 1)
    first = (other // per_group) * per_group
    member = jnp.where((channel >= first) & (channel < first + per_group), 1.0, 0.0)
    cells = 1.0 * F * H * W * per_group * n
    moments = (
        jnp.dot(
            sums,
            member.astype(jnp.float32),
            preferred_element_type=jnp.float32,
            precision=lax.Precision.HIGHEST,
        )
        / cells
    )
    mean = moments[0:1]
    var = jnp.maximum(moments[8:9] - mean * mean, 0.0)
    half_scale = lax.rsqrt(var + epsilon) * params[0] * 0.5
    half_bias = params[1] * 0.5

    column = lax.broadcasted_iota(jnp.int32, (W, C), 0)

    def activate(raw, put):
        h = (raw.astype(jnp.float32) - mean) * half_scale + half_bias
        a = h + h * jnp.tanh(h)
        put(0, jnp.where(column == 0, 0.0, pltpu.roll(a, 1, 0)).astype(jnp.bfloat16))
        put(1, a.astype(jnp.bfloat16))
        put(2, jnp.where(column == W - 1, 0.0, pltpu.roll(a, W - 1, 0)).astype(jnp.bfloat16))

    for f in range(F):
        def own_row(r, _):
            def put(k, v):
                own3[f, r, :, k * C : (k + 1) * C] = v

            activate(xv[f, r], put)
            return 0

        lax.fori_loop(0, H, own_row, 0)

    @pl.when(relays)
    def _():
        relay_in.wait_recv()
        relay_out.start()

    for c in w_copies:
        c.wait()

    def product(lhs, kt, lo=0, hi=3):
        return jnp.dot(
            lhs, wv[kt, :, lo * C : hi * C], preferred_element_type=jnp.float32
        )

    def finish(r, _):
        for f in range(F):
            out_ref[f, r] = acc[f, r + 1].astype(out_ref.dtype)
        return 0

    def own_rows(g, _):
        r0 = g * OWN_ROWS
        for kt in range(3):
            count = F - 2 + kt
            if count <= 0:
                continue
            lhs = own3[0:count, pl.ds(r0, OWN_ROWS)].reshape(count * OWN_ROWS * W, C3)
            y = product(lhs, kt)
            for kh in range(3):
                part = y[:, kh * C : (kh + 1) * C].reshape(count, OWN_ROWS, W, C)
                acc[2 - kt : 2 - kt + count, pl.ds(r0 + 2 - kh, OWN_ROWS)] += part
        return 0

    lax.fori_loop(0, H // OWN_ROWS, own_rows, 0)

    @pl.when(has_prev)
    def _():
        for i in range(2):
            halo_copy(i, 0 if i == 0 else H - 1).wait_recv()
        for side in range(2):
            @pl.when(sends_edge[side])
            def _():
                halo_edge(side).start()

    for side in range(2):
        kh = 0 if side == 0 else 2
        at = 1 if side == 0 else H

        @pl.when(gets_edge[side])
        def _():
            own_edge(side).wait_recv()
            for f in range(F):
                def put(k, v):
                    edge3[f, :, k * C : (k + 1) * C] = v

                activate(eown[side, f, 0], put)
            for kt in range(3):
                count = F - 2 + kt
                if count > 0:
                    lhs = edge3[0:count].reshape(count * W, C3)
                    acc[2 - kt : 2 - kt + count, at] += product(lhs, kt, kh, kh + 1).reshape(
                        count, W, C
                    )

    @pl.when(has_prev)
    def _():
        def halo_row(i, _):
            r = row_of(i)

            @pl.when(i >= 2)
            def _():
                halo_copy(i, r).wait_recv()

            for f in range(2):
                def put(k, v):
                    halo3[f, :, k * C : (k + 1) * C] = v

                activate(hraw[f, r], put)
            y = product(halo3[...].reshape(2 * W, C3), 0)
            z = product(halo3[1], 1)
            for kh in range(3):
                cols = slice(kh * C, (kh + 1) * C)
                acc[0, r + 2 - kh] += y[:W, cols] + z[:, cols]
                acc[1, r + 2 - kh] += y[W:, cols]

            @pl.when(i >= 2)
            def _():
                finish(i - 2, 0)

            return 0

        lax.fori_loop(0, 2, halo_row, 0)
        for side in range(2):
            kh = 0 if side == 0 else 2
            at = 1 if side == 0 else H

            @pl.when(gets_edge[side])
            def _():
                halo_edge(side).wait_recv()
                for f in range(2):
                    def put(k, v):
                        halo3[f, :, k * C : (k + 1) * C] = v

                    activate(ehalo[side, f, 0], put)
                y = product(halo3[...].reshape(2 * W, C3), 0, kh, kh + 1)
                z = product(halo3[1], 1, kh, kh + 1)
                acc[0, at] += y[:W] + z
                acc[1, at] += y[W:]

        lax.fori_loop(2, H - 1, halo_row, 0)

        r = H - 2
        for f in (1, 0):
            last_copy(f).wait_recv()

            def put(k, v):
                halo3[f, :, k * C : (k + 1) * C] = v

            activate(hraw[f, r], put)
            y = product(halo3[f], 0)
            if f == 1:
                z = product(halo3[f], 1)
                for kh in range(3):
                    acc[0, r + 2 - kh] += z[:, kh * C : (kh + 1) * C]
            for kh in range(3):
                out_ref[f, r + 1 - kh] = (
                    acc[f, r + 2 - kh] + y[:, kh * C : (kh + 1) * C]
                ).astype(out_ref.dtype)

    @pl.when(jnp.logical_not(has_prev))
    def _():
        lax.fori_loop(0, H, finish, 0)

    for d in range(1, n):
        @pl.when(jnp.logical_not(far(peer(d)["tm"], tm)))
        def _():
            stat_copy(d).wait_send()

    @pl.when(second)
    def _():
        for r in range(R):
            stat_forward(r).wait_send()

    @pl.when(relays)
    def _():
        relay_out.wait_send()

    @pl.when(has_next)
    def _():
        for i in range(H - 2):
            halo_copy(i, 0 if i == 0 else H - 1 if i == 1 else i - 1).wait_send()

        @pl.when(relayed_by)
        def _():
            relay_in.wait_send()

        @pl.when(jnp.logical_not(relayed_by))
        def _():
            halo_copy(H - 2, H - 3).wait_send()

        for f in (1, 0):
            last_copy(f).wait_send()

    for side in range(2):
        @pl.when(sends_edge[side])
        def _():
            own_edge(side).wait_send()

            @pl.when(has_prev)
            def _():
                halo_edge(side).wait_send()


def shards(T, R, inputs, norm_gain, norm_bias, conv_weight, conv_bias):
    _, F, H, W, C = inputs.shape
    n = T * R

    def pin(a):
        return pltpu.with_memory_space_constraint(a, pltpu.HBM)

    vmem = pl.BlockSpec(memory_space=pltpu.VMEM)
    hbm = pl.BlockSpec(memory_space=pltpu.HBM)
    anywhere = pl.BlockSpec(memory_space=pl.ANY)
    dma = pltpu.SemaphoreType.DMA
    out = pl.pallas_call(
        functools.partial(block_kernel, T, R),
        out_shape=jax.ShapeDtypeStruct((F, H, W, C), inputs.dtype),
        in_specs=[hbm, anywhere, anywhere, hbm, anywhere],
        out_specs=vmem,
        scratch_shapes=[
            pltpu.VMEM((3, 1, C), jnp.float32),
            dma((3,)),
            pltpu.VMEM((F, H, W, C), jnp.bfloat16),
            pltpu.VMEM((3, 3 * C, 3 * C), jnp.bfloat16),
            pltpu.VMEM((2, H, W, C), jnp.bfloat16),
            pltpu.VMEM((2, F, 1, W, C), jnp.bfloat16),
            pltpu.VMEM((2, 2, 1, W, C), jnp.bfloat16),
            pltpu.VMEM((F, H, W, 3 * C), jnp.bfloat16),
            pltpu.VMEM((2, W, 3 * C), jnp.bfloat16),
            pltpu.VMEM((F, W, 3 * C), jnp.bfloat16),
            pltpu.VMEM((F, H + 2, W, C), jnp.float32),
            pltpu.VMEM((n, 2, C), jnp.float32),
            dma((F,)),
            dma((9,)),
            dma((H + 1,)),
            dma((H + 1,)),
            dma((2,)),
            dma((2,)),
            dma((2,)),
            dma((2,)),
            dma((n,)),
            dma((n,)),
            dma((R,)),
            pltpu.VMEM((2, 1, W, C), jnp.bfloat16),
            dma((3,)),
        ],
        compiler_params=pltpu.CompilerParams(
            collective_id=0, has_side_effects=True, vmem_limit_bytes=50 * 1024 * 1024
        ),
        name="norm_conv_block",
    )(
        pin(inputs.reshape(F, H, W, C)),
        pin(norm_gain),
        pin(norm_bias),
        pin(conv_weight.reshape(3, 3, 3 * C, C)),
        pin(conv_bias),
    )
    return out.reshape(inputs.shape)


def solution(mesh):
    placed = (P("batch", "tm", "rows", None, None), P(), P(), P(), P())
    return jax.shard_map(
        functools.partial(shards, mesh.shape["tm"], mesh.shape["rows"]),
        mesh=mesh,
        in_specs=placed,
        out_specs=P("batch", "tm", "rows", None, None),
        check_vma=False,
    )
```

```python
import functools

import jax
import jax.numpy as jnp
from jax import lax
from jax.experimental import pallas as pl
from jax.experimental.pallas import tpu as pltpu
from jax.sharding import PartitionSpec as P

GROUPS = 32
MESH = pl.DeviceIdType.MESH
OWN_ROWS = 4
LAST = 128

epsilon = 1e-06


def row_chunks(H):
    return [(0, 1), (H - 1, 1)] + [(r, min(2, H - 2 - r)) for r in range(1, H - 2, 2)]


def activated(raw, mean, half_scale, half_bias, put):
    W, _ = raw.shape
    column = lax.broadcasted_iota(jnp.int32, raw.shape, 0)
    h = (raw.astype(jnp.float32) - mean) * half_scale + half_bias
    a = h + h * jnp.tanh(h)
    put(0, jnp.where(column == 0, 0.0, pltpu.roll(a, 1, 0)).astype(jnp.bfloat16))
    put(1, a.astype(jnp.bfloat16))
    put(2, jnp.where(column == W - 1, 0.0, pltpu.roll(a, W - 1, 0)).astype(jnp.bfloat16))


def block_kernel(
    T, R, x_hbm, gain_hbm, nbias_hbm, w_hbm, cbias_hbm,
    out_ref, open_rows, hlast, norms, wlast,
    params, xv, wv, hraw, eown, ehalo, own3, halo3, edge3, acc, stats, relayed,
    p_sem, x_sem, w_sem, halo_send, halo_recv, edge_sem, stat_send, stat_recv, fwd_send, relay_sem,
):
    F, H, W, C = x_hbm.shape
    C3 = 3 * C
    n = T * R
    tm = lax.axis_index("tm")
    row = lax.axis_index("rows")
    me = tm * R + row

    def peer(offset):
        other = lax.rem(me + offset, n)
        return {"tm": other // R, "rows": lax.rem(other, R)}

    def landed(ref, sem):
        pltpu.make_async_copy(ref, ref, sem).wait()

    x_copies = [pltpu.make_async_copy(x_hbm.at[f], xv.at[f], x_sem.at[f]) for f in range(F)]
    w_copies = [
        pltpu.make_async_copy(w_hbm.at[kt, kh], wv.at[kt, :, pl.ds(kh * C, C)], w_sem.at[0])
        for kt in range(3)
        for kh in range(3)
    ]
    w_copies += [
        pltpu.make_async_copy(
            w_hbm.at[0, kh, pl.ds((kw + 1) * C - LAST, LAST)],
            wlast.at[pl.ds(kw * LAST, LAST), pl.ds(kh * C, C)],
            w_sem.at[1],
        )
        for kh in range(3)
        for kw in range(3)
    ]
    p_copies = [
        pltpu.make_async_copy(p, params.at[k, 0], p_sem.at[0])
        for k, p in enumerate((gain_hbm, nbias_hbm, cbias_hbm))
    ]

    def greets(other):
        return (other["tm"] > 0) | (tm == 0) | ((tm == 1) & (other["rows"] == row))

    def knows(other):
        return (tm > 0) | (other["tm"] == 0) | ((other["tm"] == 1) & (other["rows"] == row))

    barrier = pltpu.get_barrier_semaphore()
    for d in sorted(range(1, n), key=lambda d: abs(d - (n - R))):
        other = peer(d)

        @pl.when(greets(other))
        def _():
            pl.semaphore_signal(barrier, inc=1, device_id=other, device_id_type=MESH)

    for c in x_copies + p_copies:
        c.start()

    def row_of(i):
        return jnp.where(i == 0, 0, jnp.where(i == 1, H - 1, i - 1))

    chunks = row_chunks(H)
    nc = len(chunks)
    following = {"tm": lax.rem(tm + 1, T), "rows": row}

    def halo_copy(j):
        r, size = chunks[j]
        return pltpu.make_async_remote_copy(
            src_ref=xv.at[pl.ds(F - 2, 2), pl.ds(r, size)],
            dst_ref=hraw.at[:, pl.ds(r, size)],
            send_sem=halo_send.at[0],
            recv_sem=halo_recv.at[j],
            device_id=following,
            device_id_type=MESH,
        )

    def last_copy(k):
        src, dst = (
            (xv.at[F - 1, H - 2], hraw.at[1, H - 2]),
            (xv.at[F - 2, H - 2, :, : C - LAST], hraw.at[0, H - 2, :, : C - LAST]),
            (xv.at[F - 2, H - 2, :, C - LAST :], hlast),
        )[k]
        return pltpu.make_async_remote_copy(
            src_ref=src,
            dst_ref=dst,
            send_sem=halo_send.at[0],
            recv_sem=halo_recv.at[nc + k],
            device_id=following,
            device_id_type=MESH,
        )

    relay = nc - 2
    relay_row, relay_size = chunks[relay]
    relay_in = pltpu.make_async_remote_copy(
        src_ref=xv.at[pl.ds(F - 2, 2), pl.ds(relay_row, relay_size)],
        dst_ref=relayed,
        send_sem=halo_send.at[0],
        recv_sem=relay_sem.at[0],
        device_id={"tm": T - 1, "rows": row},
        device_id_type=MESH,
    )
    relay_out = pltpu.make_async_remote_copy(
        src_ref=relayed,
        dst_ref=hraw.at[:, pl.ds(relay_row, relay_size)],
        send_sem=relay_sem.at[1],
        recv_sem=halo_recv.at[relay],
        device_id={"tm": max(T - 2, 0), "rows": row},
        device_id_type=MESH,
    )

    def edge(side, src_ref, dst_ref, sem):
        s = side if R > 2 else 0
        target = row + 1 if side == 0 else row - 1
        return pltpu.make_async_remote_copy(
            src_ref=src_ref.at[:, pl.ds(H - 1 if side == 0 else 0, 1)],
            dst_ref=dst_ref.at[side],
            send_sem=edge_sem.at[sem, s],
            recv_sem=edge_sem.at[sem + 1, s],
            device_id={"tm": tm, "rows": lax.rem(target + R, R)},
            device_id_type=MESH,
        )

    def own_edge(side):
        return edge(side, xv, eown, 0)

    def halo_edge(side):
        return edge(side, hraw, ehalo, 2)

    has_next, has_prev = tm < T - 1, tm > 0
    relays, relayed_by = (tm == T - 1) & (T == 4), (tm == T - 3) & (T == 4)
    sends_edge = (row < R - 1, row > 0)
    gets_edge = (row > 0, row < R - 1)

    def add_rows(f, carry):
        def step(r, carry):
            v = xv[f, r].astype(jnp.float32).reshape(W // 8, 8, C)
            return carry[0] + jnp.sum(v, axis=0), carry[1] + jnp.sum(v * v, axis=0)

        return lax.fori_loop(0, H, step, carry)

    carry = (jnp.zeros((8, C), jnp.float32), jnp.zeros((8, C), jnp.float32))
    for f in range(F):
        x_copies[f].wait()
        carry = add_rows(f, carry)
    stats[0, 0:1] = jnp.sum(carry[0], axis=0, keepdims=True)
    stats[0, 1:2] = jnp.sum(carry[1], axis=0, keepdims=True)

    @pl.when(has_prev)
    def _():
        pl.semaphore_wait(barrier, n - 1)

    @pl.when(jnp.logical_not(has_prev))
    def _():
        pl.semaphore_wait(barrier, R if T > 1 else R - 1)

    def stat_copy(d):
        return pltpu.make_async_remote_copy(
            src_ref=stats.at[0],
            dst_ref=stats.at[d],
            send_sem=stat_send.at[0],
            recv_sem=stat_recv.at[1 if d == R else 0],
            device_id=peer(d),
            device_id_type=MESH,
        )

    for d in range(1, n):
        @pl.when(knows(peer(d)))
        def _():
            stat_copy(d).start()

    def stat_forward(t, r):
        d = t * R + r - row
        return pltpu.make_async_remote_copy(
            src_ref=stats.at[R],
            dst_ref=stats.at[d],
            send_sem=fwd_send.at[0],
            recv_sem=stat_recv.at[0],
            device_id={"tm": t, "rows": r},
            device_id_type=MESH,
        )

    def prev_stats():
        landed(stats.at[0], stat_recv.at[1])

    @pl.when(tm == 1)
    def _():
        prev_stats()
        for t in range(1, T):
            for r in range(R):
                if t == 1:
                    @pl.when(row != r)
                    def _():
                        stat_forward(t, r).start()
                else:
                    stat_forward(t, r).start()

    @pl.when(relayed_by)
    def _():
        relay_in.start()

    @pl.when(has_next)
    def _():
        halo_copy(0).start()

    for c in w_copies:
        c.start()

    for side in range(2):
        @pl.when(sends_edge[side])
        def _():
            own_edge(side).start()

    @pl.when(has_next)
    def _():
        for j in range(1, nc):
            if j == relay:
                @pl.when(jnp.logical_not(relayed_by))
                def _():
                    halo_copy(j).start()
            else:
                halo_copy(j).start()

        for k in range(3):
            last_copy(k).start()

    landed(params, p_sem.at[0])
    for f in range(F):
        def start_acc(r, _):
            acc[f, r + 1] = xv[f, r].astype(jnp.float32) + params[2]
            return 0

        lax.fori_loop(0, H, start_acc, 0)

    @pl.when(tm != 1)
    def _():
        prev_stats()

    landed(stats.at[pl.ds(0, n - 2)], stat_recv.at[0])
    total = stats[0]
    for d in range(1, n):
        total = total + stats[d]
    sums = jnp.concatenate(
        [jnp.broadcast_to(total[0:1], (8, C)), jnp.broadcast_to(total[1:2], (8, C))], axis=0
    )
    per_group = C // GROUPS
    channel = lax.broadcasted_iota(jnp.int32, (C, C), 0)
    other = lax.broadcasted_iota(jnp.int32, (C, C), 1)
    first = (other // per_group) * per_group
    member = jnp.where((channel >= first) & (channel < first + per_group), 1.0, 0.0)
    cells = 1.0 * F * H * W * per_group * n
    moments = (
        jnp.dot(
            sums,
            member.astype(jnp.float32),
            preferred_element_type=jnp.float32,
            precision=lax.Precision.HIGHEST,
        )
        / cells
    )
    mean = moments[0:1]
    var = jnp.maximum(moments[8:9] - mean * mean, 0.0)
    half_scale = lax.rsqrt(var + epsilon) * params[0] * 0.5
    half_bias = params[1] * 0.5
    norms[0:1] = mean
    norms[1:2] = half_scale
    norms[2:3] = half_bias

    def activate(raw, put):
        activated(raw, mean, half_scale, half_bias, put)

    for f in range(F):
        def own_row(r, _):
            def put(k, v):
                own3[f, r, :, k * C : (k + 1) * C] = v

            activate(xv[f, r], put)
            return 0

        lax.fori_loop(0, H, own_row, 0)

    landed(wv, w_sem.at[0])

    def product(lhs, kt, lo=0, hi=3):
        return jnp.dot(
            lhs, wv[kt, :, lo * C : hi * C], preferred_element_type=jnp.float32
        )

    def finish(r, _):
        for f in range(F):
            out_ref[f, r] = acc[f, r + 1].astype(out_ref.dtype)
        return 0

    def own_rows(g, _):
        r0 = g * OWN_ROWS

        @pl.when(relays & (g == H // OWN_ROWS // 2))
        def _():
            relay_in.wait_recv()
            relay_out.start()

        for kt in range(3):
            count = F - 2 + kt
            if count <= 0:
                continue
            lhs = own3[0:count, pl.ds(r0, OWN_ROWS)].reshape(count * OWN_ROWS * W, C3)
            y = product(lhs, kt)
            for kh in range(3):
                part = y[:, kh * C : (kh + 1) * C].reshape(count, OWN_ROWS, W, C)
                acc[2 - kt : 2 - kt + count, pl.ds(r0 + 2 - kh, OWN_ROWS)] += part
        return 0

    lax.fori_loop(0, H // OWN_ROWS, own_rows, 0)

    @pl.when(has_prev)
    def _():
        landed(stats.at[pl.ds(0, n - 1)], stat_send.at[0])

    @pl.when(jnp.logical_not(has_prev))
    def _():
        landed(stats.at[pl.ds(0, R if T > 1 else R - 1)], stat_send.at[0])

    @pl.when(tm == 1)
    def _():
        landed(stats.at[pl.ds(0, n - R - 1)], fwd_send.at[0])

    landed(wlast, w_sem.at[1])
    for side in range(2):
        @pl.when(sends_edge[side])
        def _():
            own_edge(side).wait_send()

    @pl.when(has_prev)
    def _():
        for j in range(2):
            halo_copy(j).wait_recv()
        for side in range(2):
            @pl.when(sends_edge[side])
            def _():
                halo_edge(side).start()

    for side in range(2):
        kh = 0 if side == 0 else 2
        at = 1 if side == 0 else H

        @pl.when(gets_edge[side])
        def _():
            own_edge(side).wait_recv()
            for f in range(F):
                def put(k, v):
                    edge3[f, :, k * C : (k + 1) * C] = v

                activate(eown[side, f, 0], put)
            for kt in range(3):
                count = F - 2 + kt
                if count > 0:
                    lhs = edge3[0:count].reshape(count * W, C3)
                    acc[2 - kt : 2 - kt + count, at] += product(lhs, kt, kh, kh + 1).reshape(
                        count, W, C
                    )

    @pl.when(has_prev)
    def _():
        def halo_row(i, _):
            r = row_of(i)

            for j in range(2, nc):
                @pl.when(r == chunks[j][0])
                def _():
                    halo_copy(j).wait_recv()

            for f in range(2):
                def put(k, v):
                    halo3[f, :, k * C : (k + 1) * C] = v

                activate(hraw[f, r], put)
            y = product(halo3[...].reshape(2 * W, C3), 0)
            z = product(halo3[1], 1)
            for kh in range(3):
                cols = slice(kh * C, (kh + 1) * C)
                acc[0, r + 2 - kh] += y[:W, cols] + z[:, cols]
                acc[1, r + 2 - kh] += y[W:, cols]

            @pl.when(i >= 2)
            def _():
                finish(i - 2, 0)

            return 0

        lax.fori_loop(0, 2, halo_row, 0)
        for side in range(2):
            kh = 0 if side == 0 else 2
            at = 1 if side == 0 else H

            @pl.when(gets_edge[side])
            def _():
                halo_edge(side).wait_recv()
                for f in range(2):
                    def put(k, v):
                        halo3[f, :, k * C : (k + 1) * C] = v

                    activate(ehalo[side, f, 0], put)
                y = product(halo3[...].reshape(2 * W, C3), 0, kh, kh + 1)
                z = product(halo3[1], 1, kh, kh + 1)
                acc[0, at] += y[:W] + z
                acc[1, at] += y[W:]

        lax.fori_loop(2, H - 1, halo_row, 0)

        for side in range(2):
            @pl.when(sends_edge[side])
            def _():
                halo_edge(side).wait_send()

        @pl.when(relays)
        def _():
            relay_out.wait_send()

        r = H - 2
        last_copy(0).wait_recv()

        def put(k, v):
            halo3[1, :, k * C : (k + 1) * C] = v

        activate(hraw[1, r], put)
        y = product(halo3[1], 0)
        z = product(halo3[1], 1)
        for kh in range(3):
            cols = slice(kh * C, (kh + 1) * C)
            acc[0, r + 2 - kh] += z[:, cols]
            out_ref[1, r + 1 - kh] = (acc[1, r + 2 - kh] + y[:, cols]).astype(out_ref.dtype)

        last_copy(1).wait_recv()
        part = C - LAST

        def put_part(k, v):
            halo3[0, :, k * part : (k + 1) * part] = v

        activated(
            hraw[0, r, :, :part], mean[:, :part], half_scale[:, :part], half_bias[:, :part], put_part
        )
        weights = jnp.concatenate([wv[0, kw * C : kw * C + part] for kw in range(3)], axis=0)
        y = jnp.dot(halo3[0, :, : 3 * part], weights, preferred_element_type=jnp.float32)
        for kh in range(3):
            open_rows[2 - kh] = acc[0, r + 2 - kh] + y[:, kh * C : (kh + 1) * C]
        last_copy(2).wait_recv()

    @pl.when(jnp.logical_not(has_prev))
    def _():
        lax.fori_loop(0, H, finish, 0)

    @pl.when(has_next)
    def _():
        landed(xv.at[pl.ds(F - 2, 2)], halo_send.at[0])


def tail_kernel(rows_ref, open_rows, hlast, norms, wlast, out_hbm, lhs, closed, sem):
    _, H, W, C = rows_ref.shape
    has_prev = lax.axis_index("tm") > 0
    ready = [
        pltpu.make_async_copy(rows_ref.at[1:], out_hbm.at[1:], sem.at[0]),
        pltpu.make_async_copy(
            rows_ref.at[0, pl.ds(0, H - 3)], out_hbm.at[0, pl.ds(0, H - 3)], sem.at[1]
        ),
    ]
    for c in ready:
        c.start()
    tops = pltpu.make_async_copy(
        rows_ref.at[0, pl.ds(H - 3, 3)], out_hbm.at[0, pl.ds(H - 3, 3)], sem.at[2]
    )
    lasts = pltpu.make_async_copy(closed, out_hbm.at[0, pl.ds(H - 3, 3)], sem.at[2])

    @pl.when(jnp.logical_not(has_prev))
    def _():
        tops.start()
        tops.wait()

    @pl.when(has_prev)
    def _():
        def put(k, v):
            lhs[:, k * LAST : (k + 1) * LAST] = v

        activated(
            hlast[...], norms[0:1, C - LAST :], norms[1:2, C - LAST :], norms[2:3, C - LAST :], put
        )
        y = jnp.dot(lhs[...], wlast[...], preferred_element_type=jnp.float32)
        for kh in range(3):
            closed[2 - kh] = (open_rows[2 - kh] + y[:, kh * C : (kh + 1) * C]).astype(closed.dtype)
        lasts.start()
        lasts.wait()

    for c in ready:
        c.wait()


def shards(T, R, inputs, norm_gain, norm_bias, conv_weight, conv_bias):
    _, F, H, W, C = inputs.shape
    n = T * R

    def pin(a):
        return pltpu.with_memory_space_constraint(a, pltpu.HBM)

    vmem = pl.BlockSpec(memory_space=pltpu.VMEM)
    hbm = pl.BlockSpec(memory_space=pltpu.HBM)
    anywhere = pl.BlockSpec(memory_space=pl.ANY)
    dma = pltpu.SemaphoreType.DMA
    parts = pl.pallas_call(
        functools.partial(block_kernel, T, R),
        out_shape=[
            jax.ShapeDtypeStruct((F, H, W, C), inputs.dtype),
            jax.ShapeDtypeStruct((3, W, C), jnp.float32),
            jax.ShapeDtypeStruct((W, LAST), inputs.dtype),
            jax.ShapeDtypeStruct((8, C), jnp.float32),
            jax.ShapeDtypeStruct((3 * LAST, 3 * C), conv_weight.dtype),
        ],
        in_specs=[hbm, anywhere, anywhere, hbm, anywhere],
        out_specs=[vmem] * 5,
        scratch_shapes=[
            pltpu.VMEM((3, 1, C), jnp.float32),
            pltpu.VMEM((F, H, W, C), jnp.bfloat16),
            pltpu.VMEM((3, 3 * C, 3 * C), jnp.bfloat16),
            pltpu.VMEM((2, H, W, C), jnp.bfloat16),
            pltpu.VMEM((2, F, 1, W, C), jnp.bfloat16),
            pltpu.VMEM((2, 2, 1, W, C), jnp.bfloat16),
            pltpu.VMEM((F, H, W, 3 * C), jnp.bfloat16),
            pltpu.VMEM((2, W, 3 * C), jnp.bfloat16),
            pltpu.VMEM((F, W, 3 * C), jnp.bfloat16),
            pltpu.VMEM((F, H + 2, W, C), jnp.float32),
            pltpu.VMEM((n, 2, C), jnp.float32),
            pltpu.VMEM((2, row_chunks(H)[-2][1], W, C), jnp.bfloat16),
            dma((1,)),
            dma((F,)),
            dma((2,)),
            dma((1,)),
            dma((len(row_chunks(H)) + 3,)),
            dma((4, 2 if R > 2 else 1)),
            dma((1,)),
            dma((2,)),
            dma((1,)),
            dma((2,)),
        ],
        compiler_params=pltpu.CompilerParams(
            collective_id=0, has_side_effects=True, vmem_limit_bytes=50 * 1024 * 1024
        ),
        name="norm_conv_block",
    )(
        pin(inputs.reshape(F, H, W, C)),
        pin(norm_gain),
        pin(norm_bias),
        pin(conv_weight.reshape(3, 3, 3 * C, C)),
        pin(conv_bias),
    )
    out = pl.pallas_call(
        tail_kernel,
        out_shape=jax.ShapeDtypeStruct((F, H, W, C), inputs.dtype),
        in_specs=[vmem] * 5,
        out_specs=hbm,
        scratch_shapes=[
            pltpu.VMEM((W, 3 * LAST), jnp.bfloat16),
            pltpu.VMEM((3, W, C), inputs.dtype),
            dma((3,)),
        ],
        compiler_params=pltpu.CompilerParams(vmem_limit_bytes=8 * 1024 * 1024),
        name="last_rows",
    )(*parts)
    return out.reshape(inputs.shape)


def solution(mesh):
    placed = (P("batch", "tm", "rows", None, None), P(), P(), P(), P())
    return jax.shard_map(
        functools.partial(shards, mesh.shape["tm"], mesh.shape["rows"]),
        mesh=mesh,
        in_specs=placed,
        out_specs=P("batch", "tm", "rows", None, None),
        check_vma=False,
    )
```

```python
import functools

import jax
import jax.numpy as jnp
from jax import lax
from jax.experimental import pallas as pl
from jax.experimental.pallas import tpu as pltpu
from jax.sharding import PartitionSpec as P

GROUPS = 32
MESH = pl.DeviceIdType.MESH
OWN_ROWS = 4
LAST = 128

epsilon = 1e-06


def halo_chunks(H):
    half = (H - 1) // 2
    edges = [(1, 1, 0, 1), (0, 1, 0, 1), (0, 2, H - 1, 1)]
    newer = [(1, 1, 1, half), (1, 1, 1 + half, H - 2 - half)]
    older = [(0, 1, r, min(2, H - 2 - r)) for r in range(1, H - 2, 2)]
    return edges + newer + older


def activated(raw, mean, half_scale, half_bias, put):
    W, _ = raw.shape
    column = lax.broadcasted_iota(jnp.int32, raw.shape, 0)
    h = (raw.astype(jnp.float32) - mean) * half_scale + half_bias
    a = h + h * jnp.tanh(h)
    put(0, jnp.where(column == 0, 0.0, pltpu.roll(a, 1, 0)).astype(jnp.bfloat16))
    put(1, a.astype(jnp.bfloat16))
    put(2, jnp.where(column == W - 1, 0.0, pltpu.roll(a, W - 1, 0)).astype(jnp.bfloat16))


def block_kernel(
    T, R, x_hbm, gain_hbm, nbias_hbm, w_hbm, cbias_hbm,
    out_ref, open_rows, hlast, norms, wv,
    params, xv, hraw, eown, ehalo, own3, halo3, edge3, acc, stats, relayed, member,
    p_sem, x_sem, w_sem, halo_send, halo_recv, edge_sem, stat_send, stat_recv, relay_sem,
):
    F, H, W, C = x_hbm.shape
    C3 = 3 * C
    n = T * R
    tm = lax.axis_index("tm")
    row = lax.axis_index("rows")
    me = tm * R + row

    def peer(offset):
        other = lax.rem(me + offset, n)
        return {"tm": other // R, "rows": lax.rem(other, R)}

    def landed(ref, sem):
        pltpu.make_async_copy(ref, ref, sem).wait()

    x_copies = [pltpu.make_async_copy(x_hbm.at[f], xv.at[f], x_sem.at[0]) for f in range(F)]
    w_copies = [
        pltpu.make_async_copy(w_hbm.at[kt, kh], wv.at[kt, :, pl.ds(kh * C, C)], w_sem.at[0])
        for kt in range(3)
        for kh in range(3)
    ]
    p_copies = [
        pltpu.make_async_copy(p, params.at[k, 0], p_sem.at[0])
        for k, p in enumerate((gain_hbm, nbias_hbm, cbias_hbm))
    ]

    def lean(t):
        return (t == 0) | ((t == T - 2) & (T > 3))

    def waits(a, b):
        near = (a["tm"] == b["tm"]) | ((b["tm"] == a["tm"] + 1) & (a["rows"] == b["rows"]))
        return jnp.logical_not(lean(a["tm"])) | near

    mine = {"tm": tm, "rows": row}
    is_lean = lean(tm)
    passes_on = lean(tm - 1) & (tm > 0)
    met = R if T > 1 else R - 1

    def enter():
        @pl.when(is_lean)
        def _():
            pl.semaphore_wait(barrier, met)

        @pl.when(jnp.logical_not(is_lean))
        def _():
            pl.semaphore_wait(barrier, n - 1)

    barrier = pltpu.get_barrier_semaphore()
    for d in sorted(range(1, n), key=lambda d: abs(d - (n - R))):
        other = peer(d)

        @pl.when(waits(other, mine))
        def _():
            pl.semaphore_signal(barrier, inc=1, device_id=other, device_id_type=MESH)

        if d == n - R or n == R:
            for c in x_copies + p_copies:
                c.start()
            x_copies = p_copies = []
    for c in x_copies + p_copies:
        c.start()

    chunks = halo_chunks(H)
    nc = len(chunks)
    following = {"tm": lax.rem(tm + 1, T), "rows": row}

    def halo_copy(j):
        f, count, r, size = chunks[j]
        return pltpu.make_async_remote_copy(
            src_ref=xv.at[pl.ds(F - 2 + f, count), pl.ds(r, size)],
            dst_ref=hraw.at[pl.ds(f, count), pl.ds(r, size)],
            send_sem=halo_send.at[0],
            recv_sem=halo_recv.at[max(j - 2, 0)],
            device_id=following,
            device_id_type=MESH,
        )

    def first_half(k):
        half = pl.ds(k * (W // 2), W // 2)
        return pltpu.make_async_remote_copy(
            src_ref=xv.at[F - 1, 0, half],
            dst_ref=hraw.at[1, 0, half],
            send_sem=halo_send.at[0],
            recv_sem=halo_recv.at[0],
            device_id=following,
            device_id_type=MESH,
        )

    def last_copy(k):
        src, dst = (
            (xv.at[F - 2, H - 2, :, : C - LAST], hraw.at[0, H - 2, :, : C - LAST]),
            (xv.at[F - 2, H - 2, :, C - LAST :], hlast),
        )[k]
        return pltpu.make_async_remote_copy(
            src_ref=src,
            dst_ref=dst,
            send_sem=halo_send.at[0],
            recv_sem=halo_recv.at[nc - 2 + k],
            device_id=following,
            device_id_type=MESH,
        )

    relay = 4
    _, _, relay_row, relay_size = chunks[relay]
    relay_in = pltpu.make_async_remote_copy(
        src_ref=xv.at[pl.ds(F - 1, 1), pl.ds(relay_row, relay_size)],
        dst_ref=relayed,
        send_sem=halo_send.at[0],
        recv_sem=relay_sem.at[0],
        device_id={"tm": T - 1, "rows": row},
        device_id_type=MESH,
    )
    relay_out = pltpu.make_async_remote_copy(
        src_ref=relayed,
        dst_ref=hraw.at[pl.ds(1, 1), pl.ds(relay_row, relay_size)],
        send_sem=halo_send.at[0],
        recv_sem=halo_recv.at[relay - 2],
        device_id={"tm": max(T - 2, 0), "rows": row},
        device_id_type=MESH,
    )

    def edge(side, src_ref, dst_ref, sem):
        s = side if R > 2 else 0
        target = row + 1 if side == 0 else row - 1
        return pltpu.make_async_remote_copy(
            src_ref=src_ref.at[:, pl.ds(H - 1 if side == 0 else 0, 1)],
            dst_ref=dst_ref.at[side],
            send_sem=edge_sem.at[0, s],
            recv_sem=edge_sem.at[sem, s],
            device_id={"tm": tm, "rows": lax.rem(target + R, R)},
            device_id_type=MESH,
        )

    def own_edge(side):
        return edge(side, xv, eown, 1)

    def halo_edge(side):
        return edge(side, hraw, ehalo, 2)

    has_next, has_prev = tm < T - 1, tm > 0
    relays, relayed_by = (tm == T - 1) & (T == 4), (tm == T - 3) & (T == 4)
    sends_edge = (row < R - 1, row > 0)
    gets_edge = (row > 0, row < R - 1)

    def add_rows(f, carry):
        def step(r, carry):
            v = xv[f, r].astype(jnp.float32).reshape(W // 8, 8, C)
            return carry[0] + jnp.sum(v, axis=0), carry[1] + jnp.sum(v * v, axis=0)

        return lax.fori_loop(0, H, step, carry)

    early = is_lean & has_next
    carry = (jnp.zeros((8, C), jnp.float32), jnp.zeros((8, C), jnp.float32))
    landed(xv, x_sem.at[0])

    @pl.when(early & has_prev)
    def _():
        enter()
        first_half(0).start()

    carry = add_rows(0, carry)

    @pl.when(early & jnp.logical_not(has_prev))
    def _():
        enter()
        first_half(0).start()

    for f in range(1, F):
        carry = add_rows(f, carry)
    stats[0, 0:1] = jnp.sum(carry[0], axis=0, keepdims=True)
    stats[0, 1:2] = jnp.sum(carry[1], axis=0, keepdims=True)

    @pl.when(jnp.logical_not(early))
    def _():
        enter()

    def stat_copy(d):
        return pltpu.make_async_remote_copy(
            src_ref=stats.at[0],
            dst_ref=stats.at[d],
            send_sem=stat_send.at[0],
            recv_sem=stat_recv.at[1 if d == R else 0],
            device_id=peer(d),
            device_id_type=MESH,
        )

    for d in range(1, n):
        @pl.when(waits(mine, peer(d)))
        def _():
            stat_copy(d).start()

    def stat_forward(t, r):
        d = lax.rem((t + T + 1 - tm) * R + r - row + n, n)
        return pltpu.make_async_remote_copy(
            src_ref=stats.at[R],
            dst_ref=stats.at[d],
            send_sem=stat_send.at[0],
            recv_sem=stat_recv.at[0],
            device_id={"tm": t, "rows": r},
            device_id_type=MESH,
        )

    def prev_stats():
        landed(stats.at[0], stat_recv.at[1])

    @pl.when(has_next & jnp.logical_not(early))
    def _():
        first_half(0).start()

    @pl.when(passes_on)
    def _():
        prev_stats()
        for t in range(T):
            for r in range(R):
                @pl.when((tm != t + 1) & ((tm != t) | (row != r)))
                def _():
                    stat_forward(t, r).start()

    @pl.when(relayed_by)
    def _():
        relay_in.start()

    for c in w_copies:
        c.start()

    for side in range(2):
        @pl.when(sends_edge[side])
        def _():
            own_edge(side).start()

    @pl.when(has_next)
    def _():
        first_half(1).start()
        for j in range(1, nc):
            if j == relay:
                @pl.when(jnp.logical_not(relayed_by))
                def _():
                    halo_copy(j).start()
            else:
                halo_copy(j).start()

        for k in range(2):
            last_copy(k).start()

    landed(params, p_sem.at[0])
    per_group = C // GROUPS
    channel = lax.broadcasted_iota(jnp.int32, (C, C), 0)
    other = lax.broadcasted_iota(jnp.int32, (C, C), 1)
    first = (other // per_group) * per_group
    member[...] = jnp.where(
        (channel >= first) & (channel < first + per_group), 1.0, 0.0
    ).astype(jnp.bfloat16)
    for f in range(F):
        def start_acc(r, _):
            acc[f, r + 1] = xv[f, r].astype(jnp.float32) + params[2]
            return 0

        lax.fori_loop(0, H, start_acc, 0)

    @pl.when(jnp.logical_not(passes_on))
    def _():
        prev_stats()

    landed(stats.at[pl.ds(0, n - 2)], stat_recv.at[0])
    total = stats[0]
    for d in range(1, n):
        total = total + stats[d]
    high = total.astype(jnp.bfloat16)
    rest = total - high.astype(jnp.float32)
    middle = rest.astype(jnp.bfloat16)
    low = (rest - middle.astype(jnp.float32)).astype(jnp.bfloat16)
    pieces = [
        jnp.broadcast_to(p[k : k + 1], (16, C)) for k in range(2) for p in (high, middle, low)
    ]
    grouped = jnp.dot(
        jnp.concatenate(pieces, axis=0), member[...], preferred_element_type=jnp.float32
    )
    cells = 1.0 * F * H * W * per_group * n

    def moment(k):
        at = 48 * k
        three = grouped[at : at + 1] + grouped[at + 16 : at + 17] + grouped[at + 32 : at + 33]
        return three / cells

    moments = jnp.concatenate([moment(0), moment(1)], axis=0)
    mean = moments[0:1]
    var = jnp.maximum(moments[1:2] - mean * mean, 0.0)
    half_scale = lax.rsqrt(var + epsilon) * params[0] * 0.5
    half_bias = params[1] * 0.5
    norms[0:1] = mean
    norms[1:2] = half_scale
    norms[2:3] = half_bias

    def activate(raw, put):
        activated(raw, mean, half_scale, half_bias, put)

    for f in range(F):
        def own_row(r, _):
            def put(k, v):
                own3[f, r, :, k * C : (k + 1) * C] = v

            activate(xv[f, r], put)
            return 0

        lax.fori_loop(0, H, own_row, 0)

    landed(wv, w_sem.at[0])

    def product(lhs, kt, lo=0, hi=3):
        return jnp.dot(
            lhs, wv[kt, :, lo * C : hi * C], preferred_element_type=jnp.float32
        )

    def finish(r, _):
        for f in range(F):
            out_ref[f, r] = acc[f, r + 1].astype(out_ref.dtype)
        return 0

    def own_rows(g, _):
        r0 = g * OWN_ROWS

        @pl.when(relays & (g == H // OWN_ROWS // 2))
        def _():
            relay_in.wait_recv()
            relay_out.start()

        for kt in range(3):
            count = F - 2 + kt
            if count <= 0:
                continue
            lhs = own3[0:count, pl.ds(r0, OWN_ROWS)].reshape(count * OWN_ROWS * W, C3)
            y = product(lhs, kt)
            for kh in range(3):
                part = y[:, kh * C : (kh + 1) * C].reshape(count, OWN_ROWS, W, C)
                acc[2 - kt : 2 - kt + count, pl.ds(r0 + 2 - kh, OWN_ROWS)] += part
        return 0

    lax.fori_loop(0, H // OWN_ROWS, own_rows, 0)

    @pl.when(is_lean)
    def _():
        landed(stats.at[pl.ds(0, met)], stat_send.at[0])

    @pl.when(passes_on)
    def _():
        landed(stats.at[pl.ds(0, n - 1 + n - R - 1)], stat_send.at[0])

    @pl.when(jnp.logical_not(is_lean | passes_on))
    def _():
        landed(stats.at[pl.ds(0, n - 1)], stat_send.at[0])

    for side in range(2):
        @pl.when(sends_edge[side] & jnp.logical_not(has_prev))
        def _():
            own_edge(side).wait_send()

    @pl.when(has_prev)
    def _():
        landed(hraw.at[:, pl.ds(0, 2)], halo_recv.at[0])
        for side in range(2):
            @pl.when(sends_edge[side])
            def _():
                halo_edge(side).start()

    for side in range(2):
        kh = 0 if side == 0 else 2
        at = 1 if side == 0 else H

        @pl.when(gets_edge[side])
        def _():
            own_edge(side).wait_recv()
            for f in range(F):
                def put(k, v):
                    edge3[f, :, k * C : (k + 1) * C] = v

                activate(eown[side, f, 0], put)
            for kt in range(3):
                count = F - 2 + kt
                if count > 0:
                    lhs = edge3[0:count].reshape(count * W, C3)
                    acc[2 - kt : 2 - kt + count, at] += product(lhs, kt, kh, kh + 1).reshape(
                        count, W, C
                    )

    @pl.when(has_prev)
    def _():
        def halo_row(i, _):
            r = i * (H - 1)
            for f in range(2):
                def put(k, v):
                    halo3[f, :, k * C : (k + 1) * C] = v

                activate(hraw[f, r], put)
            y = product(halo3[...].reshape(2 * W, C3), 0)
            z = product(halo3[1], 1)
            for kh in range(3):
                cols = slice(kh * C, (kh + 1) * C)
                acc[0, r + 2 - kh] += y[:W, cols] + z[:, cols]
                acc[1, r + 2 - kh] += y[W:, cols]
            return 0

        def close(f, r):
            out_ref[f, r] = acc[f, r + 1].astype(out_ref.dtype)

        def arrive(f, r):
            for j in range(3, nc):
                if chunks[j][0] == f:
                    @pl.when(r == chunks[j][2])
                    def _():
                        halo_copy(j).wait_recv()

        def newer_row(r, _):
            arrive(1, r)

            def put(k, v):
                halo3[1, :, k * C : (k + 1) * C] = v

            activate(hraw[1, r], put)
            y = product(halo3[1], 0)
            z = product(halo3[1], 1)
            for kh in range(3):
                cols = slice(kh * C, (kh + 1) * C)
                acc[1, r + 2 - kh] += y[:, cols]
                acc[0, r + 2 - kh] += z[:, cols]
            close(1, r - 1)
            return 0

        def older_row(r, _):
            arrive(0, r)

            def put(k, v):
                halo3[0, :, k * C : (k + 1) * C] = v

            activate(hraw[0, r], put)
            y = product(halo3[0], 0)
            for kh in range(3):
                acc[0, r + 2 - kh] += y[:, kh * C : (kh + 1) * C]
            close(0, r - 1)
            return 0

        lax.fori_loop(0, 2, halo_row, 0)
        for side in range(2):
            kh = 0 if side == 0 else 2
            at = 1 if side == 0 else H

            @pl.when(gets_edge[side])
            def _():
                halo_edge(side).wait_recv()
                for f in range(2):
                    def put(k, v):
                        halo3[f, :, k * C : (k + 1) * C] = v

                    activate(ehalo[side, f, 0], put)
                y = product(halo3[...].reshape(2 * W, C3), 0, kh, kh + 1)
                z = product(halo3[1], 1, kh, kh + 1)
                acc[0, at] += y[:W] + z
                acc[1, at] += y[W:]

        lax.fori_loop(1, H - 1, newer_row, 0)
        for r in (H - 2, H - 1):
            close(1, r)

        for side in range(2):
            @pl.when(sends_edge[side])
            def _():
                s = side if R > 2 else 0
                landed(hraw.at[0, pl.ds(0, F + 2)], edge_sem.at[0, s])

        @pl.when(relays)
        def _():
            relay_out.wait_send()

        lax.fori_loop(1, H - 2, older_row, 0)

        r = H - 2
        last_copy(0).wait_recv()
        part = C - LAST

        def put_part(k, v):
            halo3[0, :, k * part : (k + 1) * part] = v

        activated(
            hraw[0, r, :, :part], mean[:, :part], half_scale[:, :part], half_bias[:, :part], put_part
        )
        weights = jnp.concatenate([wv[0, kw * C : kw * C + part] for kw in range(3)], axis=0)
        y = jnp.dot(halo3[0, :, : 3 * part], weights, preferred_element_type=jnp.float32)
        for kh in range(3):
            open_rows[2 - kh] = acc[0, r + 2 - kh] + y[:, kh * C : (kh + 1) * C]
        last_copy(1).wait_recv()

    @pl.when(jnp.logical_not(has_prev))
    def _():
        lax.fori_loop(0, H, finish, 0)

    @pl.when(has_next)
    def _():
        landed(xv.at[pl.ds(F - 2, 2)], halo_send.at[0])


def tail_kernel(F, rows_ref, open_rows, hlast, norms, wv, out_hbm, lhs, closed, sem):
    N, W, C = rows_ref.shape
    H = N // F
    has_prev = lax.axis_index("tm") > 0
    ready = [
        pltpu.make_async_copy(rows_ref.at[pl.ds(r, k)], out_hbm.at[pl.ds(r, k)], sem.at[0])
        for r, k in ((H, N - H), (0, H - 3))
        if k
    ]
    for c in ready:
        c.start()
    tops = pltpu.make_async_copy(
        rows_ref.at[pl.ds(H - 3, 3)], out_hbm.at[pl.ds(H - 3, 3)], sem.at[1]
    )
    lasts = pltpu.make_async_copy(closed, out_hbm.at[pl.ds(H - 3, 3)], sem.at[1])

    @pl.when(jnp.logical_not(has_prev))
    def _():
        tops.start()
        tops.wait()

    @pl.when(has_prev)
    def _():
        def put(k, v):
            lhs[:, k * LAST : (k + 1) * LAST] = v

        activated(
            hlast[...], norms[0:1, C - LAST :], norms[1:2, C - LAST :], norms[2:3, C - LAST :], put
        )
        weights = jnp.concatenate(
            [wv[0, (kw + 1) * C - LAST : (kw + 1) * C] for kw in range(3)], axis=0
        )
        y = jnp.dot(lhs[...], weights, preferred_element_type=jnp.float32)
        for kh in range(3):
            closed[2 - kh] = (open_rows[2 - kh] + y[:, kh * C : (kh + 1) * C]).astype(closed.dtype)
        lasts.start()
        lasts.wait()

    done = out_hbm.at[pl.ds(0, N - 3)]
    pltpu.make_async_copy(done, done, sem.at[0]).wait()


def shards(T, R, inputs, norm_gain, norm_bias, conv_weight, conv_bias):
    _, F, H, W, C = inputs.shape
    n = T * R

    def pin(a):
        return pltpu.with_memory_space_constraint(a, pltpu.HBM)

    vmem = pl.BlockSpec(memory_space=pltpu.VMEM)
    hbm = pl.BlockSpec(memory_space=pltpu.HBM)
    anywhere = pl.BlockSpec(memory_space=pl.ANY)
    dma = pltpu.SemaphoreType.DMA
    parts = pl.pallas_call(
        functools.partial(block_kernel, T, R),
        out_shape=[
            jax.ShapeDtypeStruct((F, H, W, C), inputs.dtype),
            jax.ShapeDtypeStruct((3, W, C), jnp.float32),
            jax.ShapeDtypeStruct((W, LAST), inputs.dtype),
            jax.ShapeDtypeStruct((8, C), jnp.float32),
            jax.ShapeDtypeStruct((3, 3 * C, 3 * C), conv_weight.dtype),
        ],
        in_specs=[hbm, anywhere, anywhere, hbm, anywhere],
        out_specs=[vmem] * 5,
        scratch_shapes=[
            pltpu.VMEM((3, 1, C), jnp.float32),
            pltpu.VMEM((F, H, W, C), jnp.bfloat16),
            pltpu.VMEM((2, H, W, C), jnp.bfloat16),
            pltpu.VMEM((2, F, 1, W, C), jnp.bfloat16),
            pltpu.VMEM((2, 2, 1, W, C), jnp.bfloat16),
            pltpu.VMEM((F, H, W, 3 * C), jnp.bfloat16),
            pltpu.VMEM((2, W, 3 * C), jnp.bfloat16),
            pltpu.VMEM((F, W, 3 * C), jnp.bfloat16),
            pltpu.VMEM((F, H + 2, W, C), jnp.float32),
            pltpu.VMEM((2 * n, 2, C), jnp.float32),
            pltpu.VMEM((1, halo_chunks(H)[4][3], W, C), jnp.bfloat16),
            pltpu.VMEM((C, C), jnp.bfloat16),
            dma((1,)),
            dma((1,)),
            dma((1,)),
            dma((1,)),
            dma((len(halo_chunks(H)),)),
            dma((3, 2 if R > 2 else 1)),
            dma((1,)),
            dma((2,)),
            dma((1,)),
        ],
        compiler_params=pltpu.CompilerParams(
            collective_id=0, has_side_effects=True, vmem_limit_bytes=36 * 1024 * 1024
        ),
        name="norm_conv_block",
    )(
        pin(inputs.reshape(F, H, W, C)),
        pin(norm_gain),
        pin(norm_bias),
        pin(conv_weight.reshape(3, 3, 3 * C, C)),
        pin(conv_bias),
    )
    out = pl.pallas_call(
        functools.partial(tail_kernel, F),
        out_shape=jax.ShapeDtypeStruct((F * H, W, C), inputs.dtype),
        in_specs=[vmem] * 5,
        out_specs=hbm,
        scratch_shapes=[
            pltpu.VMEM((W, 3 * LAST), jnp.bfloat16),
            pltpu.VMEM((3, W, C), inputs.dtype),
            dma((2,)),
        ],
        compiler_params=pltpu.CompilerParams(vmem_limit_bytes=4 * 1024 * 1024),
        name="last_rows",
    )(parts[0].reshape(F * H, W, C), *parts[1:])
    return out.reshape(inputs.shape)


def solution(mesh):
    placed = (P("batch", "tm", "rows", None, None), P(), P(), P(), P())
    return jax.shard_map(
        functools.partial(shards, mesh.shape["tm"], mesh.shape["rows"]),
        mesh=mesh,
        in_specs=placed,
        out_specs=P("batch", "tm", "rows", None, None),
        check_vma=False,
    )
```

```python
import functools

import jax
import jax.numpy as jnp
from jax import lax
from jax.experimental import pallas as pl
from jax.experimental.pallas import tpu as pltpu
from jax.sharding import PartitionSpec as P

GROUPS = 32
MESH = pl.DeviceIdType.MESH
OWN_ROWS = 4
LAST = 128

epsilon = 1e-06


def halo_chunks(H):
    half = (H - 1) // 2
    edges = [(1, 1, 0, 1), (0, 1, 0, 1), (0, 2, H - 1, 1)]
    newer = [(1, 1, 1, half), (1, 1, 1 + half, H - 2 - half)]
    older = [(0, 1, r, min(2, H - 2 - r)) for r in range(1, H - 2, 2)]
    return edges + newer + older


def activated(raw, mean, half_scale, half_bias, put):
    W, _ = raw.shape
    column = lax.broadcasted_iota(jnp.int32, raw.shape, 0)
    h = (raw.astype(jnp.float32) - mean) * half_scale + half_bias
    a = h + h * jnp.tanh(h)
    put(0, jnp.where(column == 0, 0.0, pltpu.roll(a, 1, 0)).astype(jnp.bfloat16))
    put(1, a.astype(jnp.bfloat16))
    put(2, jnp.where(column == W - 1, 0.0, pltpu.roll(a, W - 1, 0)).astype(jnp.bfloat16))


def block_kernel(
    T, R, x_hbm, gain_hbm, nbias_hbm, w_hbm, cbias_hbm,
    out_ref, open_rows, hlast, norms, wv,
    params, xv, hraw, eown, ehalo, own3, halo3, edge3, acc, stats, relayed, member,
    p_sem, x_sem, w_sem, halo_send, halo_recv, edge_sem, stat_send, stat_recv, relay_sem,
):
    F, H, W, C = x_hbm.shape
    C3 = 3 * C
    n = T * R
    tm = lax.axis_index("tm")
    row = lax.axis_index("rows")
    me = tm * R + row

    def peer(offset):
        other = lax.rem(me + offset, n)
        return {"tm": other // R, "rows": lax.rem(other, R)}

    def landed(ref, sem):
        pltpu.make_async_copy(ref, ref, sem).wait()

    x_copies = [pltpu.make_async_copy(x_hbm.at[f], xv.at[f], x_sem.at[0]) for f in range(F)]
    w_copies = [
        pltpu.make_async_copy(w_hbm.at[kt, kh], wv.at[kt, :, pl.ds(kh * C, C)], w_sem.at[0])
        for kt in range(3)
        for kh in range(3)
    ]
    p_copies = [
        pltpu.make_async_copy(p, params.at[k, 0], p_sem.at[0])
        for k, p in enumerate((gain_hbm, nbias_hbm, cbias_hbm))
    ]

    def lean(t):
        return (t == 0) | ((t == T - 2) & (T > 3))

    def waits(a, b):
        near = (a["tm"] == b["tm"]) | ((b["tm"] == a["tm"] + 1) & (a["rows"] == b["rows"]))
        return jnp.logical_not(lean(a["tm"])) | near

    mine = {"tm": tm, "rows": row}
    is_lean = lean(tm)
    passes_on = lean(tm - 1) & (tm > 0)
    met = R if T > 1 else R - 1

    def enter():
        @pl.when(is_lean)
        def _():
            pl.semaphore_wait(barrier, met)

        @pl.when(jnp.logical_not(is_lean))
        def _():
            pl.semaphore_wait(barrier, n - 1)

    barrier = pltpu.get_barrier_semaphore()
    for d in sorted(range(1, n), key=lambda d: abs(d - (n - R))):
        other = peer(d)

        @pl.when(waits(other, mine))
        def _():
            pl.semaphore_signal(barrier, inc=1, device_id=other, device_id_type=MESH)

        if d == n - R or n == R:
            for c in x_copies + p_copies:
                c.start()
            x_copies = p_copies = []
    for c in x_copies + p_copies:
        c.start()

    chunks = halo_chunks(H)
    nc = len(chunks)
    following = {"tm": lax.rem(tm + 1, T), "rows": row}

    def halo_copy(j):
        f, count, r, size = chunks[j]
        return pltpu.make_async_remote_copy(
            src_ref=xv.at[pl.ds(F - 2 + f, count), pl.ds(r, size)],
            dst_ref=hraw.at[pl.ds(f, count), pl.ds(r, size)],
            send_sem=halo_send.at[0],
            recv_sem=halo_recv.at[max(j - 2, 0)],
            device_id=following,
            device_id_type=MESH,
        )

    def first_half(k):
        half = pl.ds(k * (W // 2), W // 2)
        return pltpu.make_async_remote_copy(
            src_ref=xv.at[F - 1, 0, half],
            dst_ref=hraw.at[1, 0, half],
            send_sem=halo_send.at[0],
            recv_sem=halo_recv.at[0],
            device_id=following,
            device_id_type=MESH,
        )

    def last_copy(k):
        src, dst = (
            (xv.at[F - 2, H - 2, :, : C - LAST], hraw.at[0, H - 2, :, : C - LAST]),
            (xv.at[F - 2, H - 2, :, C - LAST :], hlast),
        )[k]
        return pltpu.make_async_remote_copy(
            src_ref=src,
            dst_ref=dst,
            send_sem=halo_send.at[0],
            recv_sem=halo_recv.at[nc - 2 + k],
            device_id=following,
            device_id_type=MESH,
        )

    relay = 4
    _, _, relay_row, relay_size = chunks[relay]
    relay_in = pltpu.make_async_remote_copy(
        src_ref=xv.at[pl.ds(F - 1, 1), pl.ds(relay_row, relay_size)],
        dst_ref=relayed,
        send_sem=halo_send.at[0],
        recv_sem=relay_sem.at[0],
        device_id={"tm": T - 1, "rows": row},
        device_id_type=MESH,
    )
    relay_out = pltpu.make_async_remote_copy(
        src_ref=relayed,
        dst_ref=hraw.at[pl.ds(1, 1), pl.ds(relay_row, relay_size)],
        send_sem=halo_send.at[0],
        recv_sem=halo_recv.at[relay - 2],
        device_id={"tm": max(T - 2, 0), "rows": row},
        device_id_type=MESH,
    )

    def edge(side, src_ref, dst_ref, sem):
        s = side if R > 2 else 0
        target = row + 1 if side == 0 else row - 1
        return pltpu.make_async_remote_copy(
            src_ref=src_ref.at[:, pl.ds(H - 1 if side == 0 else 0, 1)],
            dst_ref=dst_ref.at[side],
            send_sem=edge_sem.at[0, s],
            recv_sem=edge_sem.at[sem, s],
            device_id={"tm": tm, "rows": lax.rem(target + R, R)},
            device_id_type=MESH,
        )

    def own_edge(side):
        return edge(side, xv, eown, 1)

    def halo_edge(side):
        return edge(side, hraw, ehalo, 2)

    has_next, has_prev = tm < T - 1, tm > 0
    relays, relayed_by = (tm == T - 1) & (T == 4), (tm == T - 3) & (T == 4)
    sends_edge = (row < R - 1, row > 0)
    gets_edge = (row > 0, row < R - 1)

    def add_rows(f, carry):
        def step(r, carry):
            v = xv[f, r].astype(jnp.float32).reshape(W // 8, 8, C)
            return carry[0] + jnp.sum(v, axis=0), carry[1] + jnp.sum(v * v, axis=0)

        return lax.fori_loop(0, H, step, carry)

    early = is_lean & has_next
    carry = (jnp.zeros((8, C), jnp.float32), jnp.zeros((8, C), jnp.float32))
    landed(xv, x_sem.at[0])

    @pl.when(early)
    def _():
        enter()
        first_half(0).start()

    carry = add_rows(0, carry)

    for f in range(1, F):
        carry = add_rows(f, carry)
    stats[0, 0:1] = jnp.sum(carry[0], axis=0, keepdims=True)
    stats[0, 1:2] = jnp.sum(carry[1], axis=0, keepdims=True)

    @pl.when(jnp.logical_not(early))
    def _():
        enter()

    def stat_copy(d):
        return pltpu.make_async_remote_copy(
            src_ref=stats.at[0],
            dst_ref=stats.at[d],
            send_sem=stat_send.at[0],
            recv_sem=stat_recv.at[1 if d == R else 0],
            device_id=peer(d),
            device_id_type=MESH,
        )

    for d in range(1, n):
        @pl.when(waits(mine, peer(d)))
        def _():
            stat_copy(d).start()

    def stat_forward(t, r):
        d = lax.rem((t + T + 1 - tm) * R + r - row + n, n)
        return pltpu.make_async_remote_copy(
            src_ref=stats.at[R],
            dst_ref=stats.at[d],
            send_sem=stat_send.at[0],
            recv_sem=stat_recv.at[0],
            device_id={"tm": t, "rows": r},
            device_id_type=MESH,
        )

    def prev_stats():
        landed(stats.at[0], stat_recv.at[1])

    @pl.when(has_next & jnp.logical_not(early))
    def _():
        first_half(0).start()

    @pl.when(passes_on)
    def _():
        prev_stats()
        for t in range(T):
            for r in range(R):
                @pl.when((tm != t + 1) & ((tm != t) | (row != r)))
                def _():
                    stat_forward(t, r).start()

    @pl.when(relayed_by)
    def _():
        relay_in.start()

    @pl.when(has_next)
    def _():
        first_half(1).start()
        for j in range(1, nc):
            if j == relay:
                @pl.when(jnp.logical_not(relayed_by))
                def _():
                    halo_copy(j).start()
            else:
                halo_copy(j).start()

        for k in range(2):
            last_copy(k).start()

    for side in range(2):
        @pl.when(sends_edge[side])
        def _():
            own_edge(side).start()

    for c in w_copies:
        c.start()

    landed(params, p_sem.at[0])
    per_group = C // GROUPS
    channel = lax.broadcasted_iota(jnp.int32, (C, C), 0)
    other = lax.broadcasted_iota(jnp.int32, (C, C), 1)
    first = (other // per_group) * per_group
    member[...] = jnp.where(
        (channel >= first) & (channel < first + per_group), 1.0, 0.0
    ).astype(jnp.bfloat16)
    for f in range(F):
        def start_acc(r, _):
            acc[f, r + 1] = xv[f, r].astype(jnp.float32) + params[2]
            return 0

        lax.fori_loop(0, H, start_acc, 0)

    @pl.when(jnp.logical_not(passes_on))
    def _():
        prev_stats()

    landed(stats.at[pl.ds(0, n - 2)], stat_recv.at[0])
    total = stats[0]
    for d in range(1, n):
        total = total + stats[d]
    high = total.astype(jnp.bfloat16)
    rest = total - high.astype(jnp.float32)
    middle = rest.astype(jnp.bfloat16)
    low = (rest - middle.astype(jnp.float32)).astype(jnp.bfloat16)
    pieces = [
        jnp.broadcast_to(p[k : k + 1], (16, C)) for k in range(2) for p in (high, middle, low)
    ]
    grouped = jnp.dot(
        jnp.concatenate(pieces, axis=0), member[...], preferred_element_type=jnp.float32
    )
    cells = 1.0 * F * H * W * per_group * n

    def moment(k):
        at = 48 * k
        three = grouped[at : at + 1] + grouped[at + 16 : at + 17] + grouped[at + 32 : at + 33]
        return three / cells

    moments = jnp.concatenate([moment(0), moment(1)], axis=0)
    mean = moments[0:1]
    var = jnp.maximum(moments[1:2] - mean * mean, 0.0)
    half_scale = lax.rsqrt(var + epsilon) * params[0] * 0.5
    half_bias = params[1] * 0.5
    norms[0:1] = mean
    norms[1:2] = half_scale
    norms[2:3] = half_bias

    def activate(raw, put):
        activated(raw, mean, half_scale, half_bias, put)

    for f in range(F):
        def own_row(r, _):
            def put(k, v):
                own3[f, r, :, k * C : (k + 1) * C] = v

            activate(xv[f, r], put)
            return 0

        lax.fori_loop(0, H, own_row, 0)

    landed(wv, w_sem.at[0])

    def product(lhs, kt, lo=0, hi=3):
        return jnp.dot(
            lhs, wv[kt, :, lo * C : hi * C], preferred_element_type=jnp.float32
        )

    def finish(r, _):
        for f in range(F):
            out_ref[f, r] = acc[f, r + 1].astype(out_ref.dtype)
        return 0

    def own_rows(g, _):
        r0 = g * OWN_ROWS

        @pl.when(relays & (g == H // OWN_ROWS // 2))
        def _():
            relay_in.wait_recv()
            relay_out.start()

        for kt in range(3):
            count = F - 2 + kt
            if count <= 0:
                continue
            lhs = own3[0:count, pl.ds(r0, OWN_ROWS)].reshape(count * OWN_ROWS * W, C3)
            y = product(lhs, kt)
            for kh in range(3):
                part = y[:, kh * C : (kh + 1) * C].reshape(count, OWN_ROWS, W, C)
                acc[2 - kt : 2 - kt + count, pl.ds(r0 + 2 - kh, OWN_ROWS)] += part
        return 0

    lax.fori_loop(0, H // OWN_ROWS, own_rows, 0)

    @pl.when(is_lean)
    def _():
        landed(stats.at[pl.ds(0, met)], stat_send.at[0])

    @pl.when(passes_on)
    def _():
        landed(stats.at[pl.ds(0, n - 1 + n - R - 1)], stat_send.at[0])

    @pl.when(jnp.logical_not(is_lean | passes_on))
    def _():
        landed(stats.at[pl.ds(0, n - 1)], stat_send.at[0])

    for side in range(2):
        @pl.when(sends_edge[side] & jnp.logical_not(has_prev))
        def _():
            own_edge(side).wait_send()

    @pl.when(has_prev)
    def _():
        landed(hraw.at[:, pl.ds(0, 2)], halo_recv.at[0])
        for side in range(2):
            @pl.when(sends_edge[side])
            def _():
                halo_edge(side).start()

    for side in range(2):
        kh = 0 if side == 0 else 2
        at = 1 if side == 0 else H

        @pl.when(gets_edge[side])
        def _():
            own_edge(side).wait_recv()
            for f in range(F):
                def put(k, v):
                    edge3[f, :, k * C : (k + 1) * C] = v

                activate(eown[side, f, 0], put)
            for kt in range(3):
                count = F - 2 + kt
                if count > 0:
                    lhs = edge3[0:count].reshape(count * W, C3)
                    acc[2 - kt : 2 - kt + count, at] += product(lhs, kt, kh, kh + 1).reshape(
                        count, W, C
                    )

    @pl.when(has_prev)
    def _():
        def halo_row(i, _):
            r = i * (H - 1)
            for f in range(2):
                def put(k, v):
                    halo3[f, :, k * C : (k + 1) * C] = v

                activate(hraw[f, r], put)
            y = product(halo3[...].reshape(2 * W, C3), 0)
            z = product(halo3[1], 1)
            for kh in range(3):
                cols = slice(kh * C, (kh + 1) * C)
                acc[0, r + 2 - kh] += y[:W, cols] + z[:, cols]
                acc[1, r + 2 - kh] += y[W:, cols]
            return 0

        def close(f, r):
            out_ref[f, r] = acc[f, r + 1].astype(out_ref.dtype)

        def arrive(f, r):
            for j in range(3, nc):
                if chunks[j][0] == f:
                    @pl.when(r == chunks[j][2])
                    def _():
                        halo_copy(j).wait_recv()

        def newer_row(r, _):
            arrive(1, r)

            def put(k, v):
                halo3[1, :, k * C : (k + 1) * C] = v

            activate(hraw[1, r], put)
            y = product(halo3[1], 0)
            z = product(halo3[1], 1)
            for kh in range(3):
                cols = slice(kh * C, (kh + 1) * C)
                acc[1, r + 2 - kh] += y[:, cols]
                acc[0, r + 2 - kh] += z[:, cols]
            close(1, r - 1)
            return 0

        def older_row(r, _):
            arrive(0, r)

            def put(k, v):
                halo3[0, :, k * C : (k + 1) * C] = v

            activate(hraw[0, r], put)
            y = product(halo3[0], 0)
            for kh in range(3):
                acc[0, r + 2 - kh] += y[:, kh * C : (kh + 1) * C]
            close(0, r - 1)
            return 0

        lax.fori_loop(0, 2, halo_row, 0)
        for side in range(2):
            kh = 0 if side == 0 else 2
            at = 1 if side == 0 else H

            @pl.when(gets_edge[side])
            def _():
                halo_edge(side).wait_recv()
                for f in range(2):
                    def put(k, v):
                        halo3[f, :, k * C : (k + 1) * C] = v

                    activate(ehalo[side, f, 0], put)
                y = product(halo3[...].reshape(2 * W, C3), 0, kh, kh + 1)
                z = product(halo3[1], 1, kh, kh + 1)
                acc[0, at] += y[:W] + z
                acc[1, at] += y[W:]

        lax.fori_loop(1, H - 1, newer_row, 0)
        for r in (H - 2, H - 1):
            close(1, r)

        for side in range(2):
            @pl.when(sends_edge[side])
            def _():
                s = side if R > 2 else 0
                landed(hraw.at[0, pl.ds(0, F + 2)], edge_sem.at[0, s])

        @pl.when(relays)
        def _():
            relay_out.wait_send()

        lax.fori_loop(1, H - 2, older_row, 0)

        r = H - 2
        last_copy(0).wait_recv()
        part = C - LAST

        def put_part(k, v):
            halo3[0, :, k * part : (k + 1) * part] = v

        activated(
            hraw[0, r, :, :part], mean[:, :part], half_scale[:, :part], half_bias[:, :part], put_part
        )
        weights = jnp.concatenate([wv[0, kw * C : kw * C + part] for kw in range(3)], axis=0)
        y = jnp.dot(halo3[0, :, : 3 * part], weights, preferred_element_type=jnp.float32)
        for kh in range(3):
            open_rows[2 - kh] = acc[0, r + 2 - kh] + y[:, kh * C : (kh + 1) * C]
        last_copy(1).wait_recv()

    @pl.when(jnp.logical_not(has_prev))
    def _():
        lax.fori_loop(0, H, finish, 0)

    @pl.when(has_next)
    def _():
        landed(xv.at[pl.ds(F - 2, 2)], halo_send.at[0])


def tail_kernel(F, rows_ref, open_rows, hlast, norms, wv, out_hbm, lhs, closed, sem):
    N, W, C = rows_ref.shape
    H = N // F
    has_prev = lax.axis_index("tm") > 0
    ready = [
        pltpu.make_async_copy(rows_ref.at[pl.ds(r, k)], out_hbm.at[pl.ds(r, k)], sem.at[0])
        for r, k in ((H, N - H), (0, H - 3))
        if k
    ]
    for c in ready:
        c.start()
    tops = pltpu.make_async_copy(
        rows_ref.at[pl.ds(H - 3, 3)], out_hbm.at[pl.ds(H - 3, 3)], sem.at[1]
    )
    lasts = pltpu.make_async_copy(closed, out_hbm.at[pl.ds(H - 3, 3)], sem.at[1])

    @pl.when(jnp.logical_not(has_prev))
    def _():
        tops.start()
        tops.wait()

    @pl.when(has_prev)
    def _():
        def put(k, v):
            lhs[:, k * LAST : (k + 1) * LAST] = v

        activated(
            hlast[...], norms[0:1, C - LAST :], norms[1:2, C - LAST :], norms[2:3, C - LAST :], put
        )
        weights = jnp.concatenate(
            [wv[0, (kw + 1) * C - LAST : (kw + 1) * C] for kw in range(3)], axis=0
        )
        y = jnp.dot(lhs[...], weights, preferred_element_type=jnp.float32)
        for kh in range(3):
            closed[2 - kh] = (open_rows[2 - kh] + y[:, kh * C : (kh + 1) * C]).astype(closed.dtype)
        lasts.start()
        lasts.wait()

    done = out_hbm.at[pl.ds(0, N - 3)]
    pltpu.make_async_copy(done, done, sem.at[0]).wait()


def shards(T, R, inputs, norm_gain, norm_bias, conv_weight, conv_bias):
    _, F, H, W, C = inputs.shape
    n = T * R

    def pin(a):
        return pltpu.with_memory_space_constraint(a, pltpu.HBM)

    vmem = pl.BlockSpec(memory_space=pltpu.VMEM)
    hbm = pl.BlockSpec(memory_space=pltpu.HBM)
    anywhere = pl.BlockSpec(memory_space=pl.ANY)
    dma = pltpu.SemaphoreType.DMA
    parts = pl.pallas_call(
        functools.partial(block_kernel, T, R),
        out_shape=[
            jax.ShapeDtypeStruct((F, H, W, C), inputs.dtype),
            jax.ShapeDtypeStruct((3, W, C), jnp.float32),
            jax.ShapeDtypeStruct((W, LAST), inputs.dtype),
            jax.ShapeDtypeStruct((8, C), jnp.float32),
            jax.ShapeDtypeStruct((3, 3 * C, 3 * C), conv_weight.dtype),
        ],
        in_specs=[hbm, anywhere, anywhere, hbm, anywhere],
        out_specs=[vmem] * 5,
        scratch_shapes=[
            pltpu.VMEM((3, 1, C), jnp.float32),
            pltpu.VMEM((F, H, W, C), jnp.bfloat16),
            pltpu.VMEM((2, H, W, C), jnp.bfloat16),
            pltpu.VMEM((2, F, 1, W, C), jnp.bfloat16),
            pltpu.VMEM((2, 2, 1, W, C), jnp.bfloat16),
            pltpu.VMEM((F, H, W, 3 * C), jnp.bfloat16),
            pltpu.VMEM((2, W, 3 * C), jnp.bfloat16),
            pltpu.VMEM((F, W, 3 * C), jnp.bfloat16),
            pltpu.VMEM((F, H + 2, W, C), jnp.float32),
            pltpu.VMEM((2 * n, 2, C), jnp.float32),
            pltpu.VMEM((1, halo_chunks(H)[4][3], W, C), jnp.bfloat16),
            pltpu.VMEM((C, C), jnp.bfloat16),
            dma((1,)),
            dma((1,)),
            dma((1,)),
            dma((1,)),
            dma((len(halo_chunks(H)),)),
            dma((3, 2 if R > 2 else 1)),
            dma((1,)),
            dma((2,)),
            dma((1,)),
        ],
        compiler_params=pltpu.CompilerParams(
            collective_id=0, has_side_effects=True, vmem_limit_bytes=36 * 1024 * 1024
        ),
        name="norm_conv_block",
    )(
        pin(inputs.reshape(F, H, W, C)),
        pin(norm_gain),
        pin(norm_bias),
        pin(conv_weight.reshape(3, 3, 3 * C, C)),
        pin(conv_bias),
    )
    out = pl.pallas_call(
        functools.partial(tail_kernel, F),
        out_shape=jax.ShapeDtypeStruct((F * H, W, C), inputs.dtype),
        in_specs=[vmem] * 5,
        out_specs=hbm,
        scratch_shapes=[
            pltpu.VMEM((W, 3 * LAST), jnp.bfloat16),
            pltpu.VMEM((3, W, C), inputs.dtype),
            dma((2,)),
        ],
        compiler_params=pltpu.CompilerParams(vmem_limit_bytes=4 * 1024 * 1024),
        name="last_rows",
    )(parts[0].reshape(F * H, W, C), *parts[1:])
    return out.reshape(inputs.shape)


def solution(mesh):
    placed = (P("batch", "tm", "rows", None, None), P(), P(), P(), P())
    return jax.shard_map(
        functools.partial(shards, mesh.shape["tm"], mesh.shape["rows"]),
        mesh=mesh,
        in_specs=placed,
        out_specs=P("batch", "tm", "rows", None, None),
        check_vma=False,
    )
```

```python
import functools

import jax
import jax.numpy as jnp
from jax import lax
from jax.experimental import pallas as pl
from jax.experimental.pallas import tpu as pltpu
from jax.sharding import PartitionSpec as P

GROUPS = 32
MESH = pl.DeviceIdType.MESH
OWN_ROWS = 4
LAST = 128

epsilon = 1e-06


def halo_chunks(H):
    half = (H - 1) // 2
    edges = [(1, 1, 0, 1), (0, 1, 0, 1), (0, 2, H - 1, 1)]
    newer = [(1, 1, 1, half), (1, 1, 1 + half, H - 2 - half)]
    older = [(0, 1, r, min(2, H - 2 - r)) for r in range(1, H - 2, 2)]
    return edges + newer + older


def activated(raw, mean, half_scale, half_bias, put):
    W, _ = raw.shape
    column = lax.broadcasted_iota(jnp.int32, raw.shape, 0)
    h = (raw.astype(jnp.float32) - mean) * half_scale + half_bias
    a = h + h * jnp.tanh(h)
    put(0, jnp.where(column == 0, 0.0, pltpu.roll(a, 1, 0)).astype(jnp.bfloat16))
    put(1, a.astype(jnp.bfloat16))
    put(2, jnp.where(column == W - 1, 0.0, pltpu.roll(a, W - 1, 0)).astype(jnp.bfloat16))


def block_kernel(
    T, R, x_hbm, gain_hbm, nbias_hbm, w_hbm, cbias_hbm,
    out_ref, open_rows, hlast, norms, wv,
    params, xv, hraw, eown, ehalo, own3, halo3, edge3, acc, stats, relayed, member,
    p_sem, x_sem, w_sem, halo_send, halo_recv, edge_sem, stat_send, stat_recv, relay_sem,
):
    F, H, W, C = x_hbm.shape
    C3 = 3 * C
    n = T * R
    tm = lax.axis_index("tm")
    row = lax.axis_index("rows")
    me = tm * R + row

    def peer(offset):
        other = lax.rem(me + offset, n)
        return {"tm": other // R, "rows": lax.rem(other, R)}

    def landed(ref, sem):
        pltpu.make_async_copy(ref, ref, sem).wait()

    x_copies = [pltpu.make_async_copy(x_hbm.at[f], xv.at[f], x_sem.at[0]) for f in range(F)]
    w_copies = [
        pltpu.make_async_copy(w_hbm.at[kt, kh], wv.at[kt, :, pl.ds(kh * C, C)], w_sem.at[0])
        for kt in range(3)
        for kh in range(3)
    ]
    p_copies = [
        pltpu.make_async_copy(p, params.at[k, 0], p_sem.at[0])
        for k, p in enumerate((gain_hbm, nbias_hbm, cbias_hbm))
    ]

    def lean(t):
        return (t == 0) | ((t == T - 2) & (T > 3))

    def waits(a, b):
        near = (a["tm"] == b["tm"]) | ((b["tm"] == a["tm"] + 1) & (a["rows"] == b["rows"]))
        return jnp.logical_not(lean(a["tm"])) | near

    mine = {"tm": tm, "rows": row}
    is_lean = lean(tm)
    passes_on = lean(tm - 1) & (tm > 0)
    met = R if T > 1 else R - 1

    def enter():
        @pl.when(is_lean)
        def _():
            pl.semaphore_wait(barrier, met)

        @pl.when(jnp.logical_not(is_lean))
        def _():
            pl.semaphore_wait(barrier, n - 1)

    barrier = pltpu.get_barrier_semaphore()
    for d in sorted(range(1, n), key=lambda d: abs(d - (n - R))):
        other = peer(d)

        @pl.when(waits(other, mine))
        def _():
            pl.semaphore_signal(barrier, inc=1, device_id=other, device_id_type=MESH)

        if d == n - R or n == R:
            for c in x_copies + p_copies:
                c.start()
            x_copies = p_copies = []
    for c in x_copies + p_copies:
        c.start()

    chunks = halo_chunks(H)
    nc = len(chunks)
    following = {"tm": lax.rem(tm + 1, T), "rows": row}

    def halo_copy(j):
        f, count, r, size = chunks[j]
        return pltpu.make_async_remote_copy(
            src_ref=xv.at[pl.ds(F - 2 + f, count), pl.ds(r, size)],
            dst_ref=hraw.at[pl.ds(f, count), pl.ds(r, size)],
            send_sem=halo_send.at[0],
            recv_sem=halo_recv.at[max(j - 2, 0)],
            device_id=following,
            device_id_type=MESH,
        )

    def first_row(k):
        cut = 3 * W // 4
        part = pl.ds(0, cut) if k == 0 else pl.ds(cut, W - cut)
        return pltpu.make_async_remote_copy(
            src_ref=xv.at[F - 1, 0, part],
            dst_ref=hraw.at[1, 0, part],
            send_sem=halo_send.at[0],
            recv_sem=halo_recv.at[0],
            device_id=following,
            device_id_type=MESH,
        )

    def last_copy(k):
        src, dst = (
            (xv.at[F - 2, H - 2, :, : C - LAST], hraw.at[0, H - 2, :, : C - LAST]),
            (xv.at[F - 2, H - 2, :, C - LAST :], hlast),
        )[k]
        return pltpu.make_async_remote_copy(
            src_ref=src,
            dst_ref=dst,
            send_sem=halo_send.at[0],
            recv_sem=halo_recv.at[nc - 2 + k],
            device_id=following,
            device_id_type=MESH,
        )

    relay = 4
    _, _, relay_row, relay_size = chunks[relay]
    relay_in = pltpu.make_async_remote_copy(
        src_ref=xv.at[pl.ds(F - 1, 1), pl.ds(relay_row, relay_size)],
        dst_ref=relayed,
        send_sem=halo_send.at[0],
        recv_sem=relay_sem.at[0],
        device_id={"tm": T - 1, "rows": row},
        device_id_type=MESH,
    )
    relay_out = pltpu.make_async_remote_copy(
        src_ref=relayed,
        dst_ref=hraw.at[pl.ds(1, 1), pl.ds(relay_row, relay_size)],
        send_sem=halo_send.at[0],
        recv_sem=halo_recv.at[relay - 2],
        device_id={"tm": max(T - 2, 0), "rows": row},
        device_id_type=MESH,
    )

    def edge(side, src_ref, dst_ref, sem):
        s = side if R > 2 else 0
        target = row + 1 if side == 0 else row - 1
        return pltpu.make_async_remote_copy(
            src_ref=src_ref.at[:, pl.ds(H - 1 if side == 0 else 0, 1)],
            dst_ref=dst_ref.at[side],
            send_sem=edge_sem.at[0, s],
            recv_sem=edge_sem.at[sem, s],
            device_id={"tm": tm, "rows": lax.rem(target + R, R)},
            device_id_type=MESH,
        )

    def own_edge(side):
        return edge(side, xv, eown, 1)

    def halo_edge(side):
        return edge(side, hraw, ehalo, 2)

    has_next, has_prev = tm < T - 1, tm > 0
    relays, relayed_by = (tm == T - 1) & (T == 4), (tm == T - 3) & (T == 4)
    sends_edge = (row < R - 1, row > 0)
    gets_edge = (row > 0, row < R - 1)

    def add_rows(f, carry):
        def step(r, carry):
            v = xv[f, r].astype(jnp.float32).reshape(W // 8, 8, C)
            return carry[0] + jnp.sum(v, axis=0), carry[1] + jnp.sum(v * v, axis=0)

        return lax.fori_loop(0, H, step, carry)

    early = is_lean & has_next
    carry = (jnp.zeros((8, C), jnp.float32), jnp.zeros((8, C), jnp.float32))
    landed(xv, x_sem.at[0])

    @pl.when(early)
    def _():
        enter()
        first_row(0).start()

    carry = add_rows(0, carry)

    for f in range(1, F):
        carry = add_rows(f, carry)
    stats[0, 0:1] = jnp.sum(carry[0], axis=0, keepdims=True)
    stats[0, 1:2] = jnp.sum(carry[1], axis=0, keepdims=True)

    @pl.when(jnp.logical_not(early))
    def _():
        enter()

    def stat_copy(d):
        return pltpu.make_async_remote_copy(
            src_ref=stats.at[0],
            dst_ref=stats.at[d],
            send_sem=stat_send.at[0],
            recv_sem=stat_recv.at[1 if d == R else 0],
            device_id=peer(d),
            device_id_type=MESH,
        )

    for d in range(1, n):
        @pl.when(waits(mine, peer(d)))
        def _():
            stat_copy(d).start()

    def stat_forward(t, r):
        d = lax.rem((t + T + 1 - tm) * R + r - row + n, n)
        return pltpu.make_async_remote_copy(
            src_ref=stats.at[R],
            dst_ref=stats.at[d],
            send_sem=stat_send.at[0],
            recv_sem=stat_recv.at[0],
            device_id={"tm": t, "rows": r},
            device_id_type=MESH,
        )

    def prev_stats():
        landed(stats.at[0], stat_recv.at[1])

    @pl.when(has_next & jnp.logical_not(early))
    def _():
        first_row(0).start()

    @pl.when(passes_on)
    def _():
        prev_stats()
        for t in range(T):
            for r in range(R):
                @pl.when((tm != t + 1) & ((tm != t) | (row != r)))
                def _():
                    stat_forward(t, r).start()

    @pl.when(relayed_by)
    def _():
        relay_in.start()

    @pl.when(has_next)
    def _():
        first_row(1).start()
        for j in range(1, nc):
            if j == relay:
                @pl.when(jnp.logical_not(relayed_by))
                def _():
                    halo_copy(j).start()
            else:
                halo_copy(j).start()

        for k in range(2):
            last_copy(k).start()

    for side in range(2):
        @pl.when(sends_edge[side])
        def _():
            own_edge(side).start()

    for c in w_copies:
        c.start()

    landed(params, p_sem.at[0])
    per_group = C // GROUPS
    channel = lax.broadcasted_iota(jnp.int32, (C, C), 0)
    other = lax.broadcasted_iota(jnp.int32, (C, C), 1)
    first = (other // per_group) * per_group
    member[...] = jnp.where(
        (channel >= first) & (channel < first + per_group), 1.0, 0.0
    ).astype(jnp.bfloat16)
    for f in range(F):
        def start_acc(r, _):
            acc[f, r + 1] = xv[f, r].astype(jnp.float32) + params[2]
            return 0

        lax.fori_loop(0, H, start_acc, 0)

    @pl.when(jnp.logical_not(passes_on))
    def _():
        prev_stats()

    landed(stats.at[pl.ds(0, n - 2)], stat_recv.at[0])
    total = stats[0]
    for d in range(1, n):
        total = total + stats[d]
    high = total.astype(jnp.bfloat16)
    rest = total - high.astype(jnp.float32)
    middle = rest.astype(jnp.bfloat16)
    low = (rest - middle.astype(jnp.float32)).astype(jnp.bfloat16)
    pieces = [
        jnp.broadcast_to(p[k : k + 1], (16, C)) for k in range(2) for p in (high, middle, low)
    ]
    grouped = jnp.dot(
        jnp.concatenate(pieces, axis=0), member[...], preferred_element_type=jnp.float32
    )
    cells = 1.0 * F * H * W * per_group * n

    def moment(k):
        at = 48 * k
        three = grouped[at : at + 1] + grouped[at + 16 : at + 17] + grouped[at + 32 : at + 33]
        return three / cells

    moments = jnp.concatenate([moment(0), moment(1)], axis=0)
    mean = moments[0:1]
    var = jnp.maximum(moments[1:2] - mean * mean, 0.0)
    half_scale = lax.rsqrt(var + epsilon) * params[0] * 0.5
    half_bias = params[1] * 0.5
    norms[0:1] = mean
    norms[1:2] = half_scale
    norms[2:3] = half_bias

    def activate(raw, put):
        activated(raw, mean, half_scale, half_bias, put)

    for f in range(F):
        def own_row(r, _):
            def put(k, v):
                own3[f, r, :, k * C : (k + 1) * C] = v

            activate(xv[f, r], put)
            return 0

        lax.fori_loop(0, H, own_row, 0)

    landed(wv, w_sem.at[0])

    def product(lhs, kt, lo=0, hi=3):
        return jnp.dot(
            lhs, wv[kt, :, lo * C : hi * C], preferred_element_type=jnp.float32
        )

    def finish(r, _):
        for f in range(F):
            out_ref[f, r] = acc[f, r + 1].astype(out_ref.dtype)
        return 0

    def own_rows(g, _):
        r0 = g * OWN_ROWS

        @pl.when(relays & (g == H // OWN_ROWS // 2))
        def _():
            relay_in.wait_recv()
            relay_out.start()

        for kt in range(3):
            count = F - 2 + kt
            if count <= 0:
                continue
            lhs = own3[0:count, pl.ds(r0, OWN_ROWS)].reshape(count * OWN_ROWS * W, C3)
            y = product(lhs, kt)
            for kh in range(3):
                part = y[:, kh * C : (kh + 1) * C].reshape(count, OWN_ROWS, W, C)
                acc[2 - kt : 2 - kt + count, pl.ds(r0 + 2 - kh, OWN_ROWS)] += part
        return 0

    lax.fori_loop(0, H // OWN_ROWS, own_rows, 0)

    @pl.when(is_lean)
    def _():
        landed(stats.at[pl.ds(0, met)], stat_send.at[0])

    @pl.when(passes_on)
    def _():
        landed(stats.at[pl.ds(0, n - 1 + n - R - 1)], stat_send.at[0])

    @pl.when(jnp.logical_not(is_lean | passes_on))
    def _():
        landed(stats.at[pl.ds(0, n - 1)], stat_send.at[0])

    for side in range(2):
        @pl.when(sends_edge[side] & jnp.logical_not(has_prev))
        def _():
            own_edge(side).wait_send()

    @pl.when(has_prev)
    def _():
        landed(hraw.at[:, pl.ds(0, 2)], halo_recv.at[0])
        for side in range(2):
            @pl.when(sends_edge[side])
            def _():
                halo_edge(side).start()

    for side in range(2):
        kh = 0 if side == 0 else 2
        at = 1 if side == 0 else H

        @pl.when(gets_edge[side])
        def _():
            own_edge(side).wait_recv()
            for f in range(F):
                def put(k, v):
                    edge3[f, :, k * C : (k + 1) * C] = v

                activate(eown[side, f, 0], put)
            for kt in range(3):
                count = F - 2 + kt
                if count > 0:
                    lhs = edge3[0:count].reshape(count * W, C3)
                    acc[2 - kt : 2 - kt + count, at] += product(lhs, kt, kh, kh + 1).reshape(
                        count, W, C
                    )

    @pl.when(has_prev)
    def _():
        def halo_row(i, _):
            r = i * (H - 1)
            for f in range(2):
                def put(k, v):
                    halo3[f, :, k * C : (k + 1) * C] = v

                activate(hraw[f, r], put)
            y = product(halo3[...].reshape(2 * W, C3), 0)
            z = product(halo3[1], 1)
            for kh in range(3):
                cols = slice(kh * C, (kh + 1) * C)
                acc[0, r + 2 - kh] += y[:W, cols] + z[:, cols]
                acc[1, r + 2 - kh] += y[W:, cols]
            return 0

        def close(f, r):
            out_ref[f, r] = acc[f, r + 1].astype(out_ref.dtype)

        def arrive(f, r):
            for j in range(3, nc):
                if chunks[j][0] == f:
                    @pl.when(r == chunks[j][2])
                    def _():
                        halo_copy(j).wait_recv()

        def newer_row(r, _):
            arrive(1, r)

            def put(k, v):
                halo3[1, :, k * C : (k + 1) * C] = v

            activate(hraw[1, r], put)
            y = product(halo3[1], 0)
            z = product(halo3[1], 1)
            for kh in range(3):
                cols = slice(kh * C, (kh + 1) * C)
                acc[1, r + 2 - kh] += y[:, cols]
                acc[0, r + 2 - kh] += z[:, cols]
            close(1, r - 1)
            return 0

        def older_row(r, _):
            arrive(0, r)

            def put(k, v):
                halo3[0, :, k * C : (k + 1) * C] = v

            activate(hraw[0, r], put)
            y = product(halo3[0], 0)
            for kh in range(3):
                acc[0, r + 2 - kh] += y[:, kh * C : (kh + 1) * C]
            close(0, r - 1)
            return 0

        lax.fori_loop(0, 2, halo_row, 0)
        for side in range(2):
            kh = 0 if side == 0 else 2
            at = 1 if side == 0 else H

            @pl.when(gets_edge[side])
            def _():
                halo_edge(side).wait_recv()
                for f in range(2):
                    def put(k, v):
                        halo3[f, :, k * C : (k + 1) * C] = v

                    activate(ehalo[side, f, 0], put)
                y = product(halo3[...].reshape(2 * W, C3), 0, kh, kh + 1)
                z = product(halo3[1], 1, kh, kh + 1)
                acc[0, at] += y[:W] + z
                acc[1, at] += y[W:]

        lax.fori_loop(1, H - 1, newer_row, 0)
        for r in (H - 2, H - 1):
            close(1, r)

        for side in range(2):
            @pl.when(sends_edge[side])
            def _():
                s = side if R > 2 else 0
                landed(hraw.at[0, pl.ds(0, F + 2)], edge_sem.at[0, s])

        @pl.when(relays)
        def _():
            relay_out.wait_send()

        lax.fori_loop(1, H - 2, older_row, 0)

        r = H - 2
        last_copy(0).wait_recv()
        part = C - LAST

        def put_part(k, v):
            halo3[0, :, k * part : (k + 1) * part] = v

        activated(
            hraw[0, r, :, :part], mean[:, :part], half_scale[:, :part], half_bias[:, :part], put_part
        )
        weights = jnp.concatenate([wv[0, kw * C : kw * C + part] for kw in range(3)], axis=0)
        y = jnp.dot(halo3[0, :, : 3 * part], weights, preferred_element_type=jnp.float32)
        for kh in range(3):
            open_rows[2 - kh] = acc[0, r + 2 - kh] + y[:, kh * C : (kh + 1) * C]
        last_copy(1).wait_recv()

    @pl.when(jnp.logical_not(has_prev))
    def _():
        lax.fori_loop(0, H, finish, 0)

    @pl.when(has_next)
    def _():
        landed(xv.at[pl.ds(F - 2, 2)], halo_send.at[0])


def tail_kernel(F, rows_ref, open_rows, hlast, norms, wv, out_hbm, lhs, closed, sem):
    N, W, C = rows_ref.shape
    H = N // F
    has_prev = lax.axis_index("tm") > 0
    ready = [
        pltpu.make_async_copy(rows_ref.at[pl.ds(r, k)], out_hbm.at[pl.ds(r, k)], sem.at[0])
        for r, k in ((H, N - H), (0, H - 3))
        if k
    ]
    for c in ready:
        c.start()
    tops = pltpu.make_async_copy(
        rows_ref.at[pl.ds(H - 3, 3)], out_hbm.at[pl.ds(H - 3, 3)], sem.at[1]
    )
    lasts = pltpu.make_async_copy(closed, out_hbm.at[pl.ds(H - 3, 3)], sem.at[1])

    @pl.when(jnp.logical_not(has_prev))
    def _():
        tops.start()
        tops.wait()

    @pl.when(has_prev)
    def _():
        def put(k, v):
            lhs[:, k * LAST : (k + 1) * LAST] = v

        activated(
            hlast[...], norms[0:1, C - LAST :], norms[1:2, C - LAST :], norms[2:3, C - LAST :], put
        )
        weights = jnp.concatenate(
            [wv[0, (kw + 1) * C - LAST : (kw + 1) * C] for kw in range(3)], axis=0
        )
        y = jnp.dot(lhs[...], weights, preferred_element_type=jnp.float32)
        for kh in range(3):
            closed[2 - kh] = (open_rows[2 - kh] + y[:, kh * C : (kh + 1) * C]).astype(closed.dtype)
        lasts.start()
        lasts.wait()

    done = out_hbm.at[pl.ds(0, N - 3)]
    pltpu.make_async_copy(done, done, sem.at[0]).wait()


def shards(T, R, inputs, norm_gain, norm_bias, conv_weight, conv_bias):
    _, F, H, W, C = inputs.shape
    n = T * R

    def pin(a):
        return pltpu.with_memory_space_constraint(a, pltpu.HBM)

    vmem = pl.BlockSpec(memory_space=pltpu.VMEM)
    hbm = pl.BlockSpec(memory_space=pltpu.HBM)
    anywhere = pl.BlockSpec(memory_space=pl.ANY)
    dma = pltpu.SemaphoreType.DMA
    parts = pl.pallas_call(
        functools.partial(block_kernel, T, R),
        out_shape=[
            jax.ShapeDtypeStruct((F, H, W, C), inputs.dtype),
            jax.ShapeDtypeStruct((3, W, C), jnp.float32),
            jax.ShapeDtypeStruct((W, LAST), inputs.dtype),
            jax.ShapeDtypeStruct((8, C), jnp.float32),
            jax.ShapeDtypeStruct((3, 3 * C, 3 * C), conv_weight.dtype),
        ],
        in_specs=[hbm, anywhere, anywhere, hbm, anywhere],
        out_specs=[vmem] * 5,
        scratch_shapes=[
            pltpu.VMEM((3, 1, C), jnp.float32),
            pltpu.VMEM((F, H, W, C), jnp.bfloat16),
            pltpu.VMEM((2, H, W, C), jnp.bfloat16),
            pltpu.VMEM((2, F, 1, W, C), jnp.bfloat16),
            pltpu.VMEM((2, 2, 1, W, C), jnp.bfloat16),
            pltpu.VMEM((F, H, W, 3 * C), jnp.bfloat16),
            pltpu.VMEM((2, W, 3 * C), jnp.bfloat16),
            pltpu.VMEM((F, W, 3 * C), jnp.bfloat16),
            pltpu.VMEM((F, H + 2, W, C), jnp.float32),
            pltpu.VMEM((2 * n, 2, C), jnp.float32),
            pltpu.VMEM((1, halo_chunks(H)[4][3], W, C), jnp.bfloat16),
            pltpu.VMEM((C, C), jnp.bfloat16),
            dma((1,)),
            dma((1,)),
            dma((1,)),
            dma((1,)),
            dma((len(halo_chunks(H)),)),
            dma((3, 2 if R > 2 else 1)),
            dma((1,)),
            dma((2,)),
            dma((1,)),
        ],
        compiler_params=pltpu.CompilerParams(
            collective_id=0, has_side_effects=True, vmem_limit_bytes=36 * 1024 * 1024
        ),
        name="norm_conv_block",
    )(
        pin(inputs.reshape(F, H, W, C)),
        pin(norm_gain),
        pin(norm_bias),
        pin(conv_weight.reshape(3, 3, 3 * C, C)),
        pin(conv_bias),
    )
    out = pl.pallas_call(
        functools.partial(tail_kernel, F),
        out_shape=jax.ShapeDtypeStruct((F * H, W, C), inputs.dtype),
        in_specs=[vmem] * 5,
        out_specs=hbm,
        scratch_shapes=[
            pltpu.VMEM((W, 3 * LAST), jnp.bfloat16),
            pltpu.VMEM((3, W, C), inputs.dtype),
            dma((2,)),
        ],
        compiler_params=pltpu.CompilerParams(vmem_limit_bytes=4 * 1024 * 1024),
        name="last_rows",
    )(parts[0].reshape(F * H, W, C), *parts[1:])
    return out.reshape(inputs.shape)


def solution(mesh):
    placed = (P("batch", "tm", "rows", None, None), P(), P(), P(), P())
    return jax.shard_map(
        functools.partial(shards, mesh.shape["tm"], mesh.shape["rows"]),
        mesh=mesh,
        in_specs=placed,
        out_specs=P("batch", "tm", "rows", None, None),
        check_vma=False,
    )
```
